32 devices in a mesh: row: 4 (over y, x), col: 8 (over z, core).
Axes of the slice: x: 2, y: 2, z: 4, core: 2. Of those that a mesh axis runs over, the one named last changes fastest.
Arguments:
- patches: bfloat16 [32, 128, 768], P('row', 'col'), may hold values from -6 to 6
- w_patch: bfloat16 [768, 6144], replicated, may hold values from -0.21875 to 0.21875
- patch_bias: bfloat16 [6144], replicated, may hold values from -5 to 5
- ln_gain: bfloat16 [6144], replicated, may hold values from 0.5 to 1.5
- w_qkv: bfloat16 [6144, 3, 48, 128], P(None, None, 'col'), may hold values from -1 to 1
- qk_gain: float32 [2, 48, 128], P(None, 'col'), may hold values from 0 to 6, as said below
- w_out: bfloat16 [48, 128, 6144], P('col', None, 'row'), may hold values from -0.078125 to 0.078125
Outputs:
- attn_branch: bfloat16 [4096, 6144], P(('row', 'col'))
The draws below stay inside these ranges and needn't reach their ends.
Inputs may be any that keep to these rules, and one draw needn't show every extreme that they name: `qk_gain`: positive gains.
All inputs are finite; a program needn't handle non-finite values.
Results may differ from the reference program's by a relative error of at most 0.015.
Values may be sent and summed in bfloat16 or wider, within the bound.
A program may use at most 320 MiB of HBM per device.

```python
import math
import jax
import jax.numpy as jnp
from jax import lax

D = 6144
H = 48
HD = 128
PATCH_IN = 768
GW = 128
GH = 32
N_COL = 8


def draw_patches(key, part):
    key_one = jax.random.fold_in(key, 0)
    result = jnp.clip(jax.random.normal(key_one, (GH, GW, PATCH_IN), jnp.float32), -6.0, 6.0)
    return result.astype(jnp.bfloat16)


def draw_w_qkv(key, part):
    key_weight = jax.random.fold_in(key, 0)
    raw_draw = jnp.clip(jax.random.normal(key_weight, (D, 3, H, HD), jnp.float32), -6.0, 6.0) * D ** (-0.5)
    return raw_draw.astype(jnp.bfloat16)


def draw_qk_gain(key, part):
    key_head, key_dim = jax.random.split(key, 2)
    head_scale = jnp.exp(jax.random.uniform(key_head, (2, H, 1), jnp.float32, 0.5, 1.5))
    gains = head_scale * (1.0 + 0.1 * jnp.clip(jax.random.normal(key_dim, (2, H, HD), jnp.float32), -3.0, 3.0))
    return gains.astype(jnp.float32)


def shard_levels(key, extent, cuts, smallest, largest):
    def one(dim, shards_of):
        heights = jax.random.uniform(jax.random.fold_in(jax.random.fold_in(key, 6), dim), (shards_of,), jnp.float32, smallest / len(cuts), largest / len(cuts))
        return jnp.repeat(jnp.exp(heights), extent[dim] // shards_of).reshape((-1,) + (1,) * (len(extent) - dim - 1))

    gain = one(*cuts[0])
    for cut in cuts[1:]:
        gain = gain * one(*cut)
    return gain


def centred(stream_key, dims, spread, limit, pieces=(), held_as=jnp.bfloat16):
    entries = jax.random.normal(stream_key, dims, jnp.float32) * spread
    if len(pieces) > 0:
        entries = shard_levels(stream_key, dims, pieces, -0.22, 0.18) * entries
    return jnp.clip(entries, min=-limit, max=limit).astype(held_as)


def setup_inputs(seed: int = 0) -> dict:
    arg_keys = jax.random.split(jax.random.key(seed), 8)
    patches = draw_patches(jax.random.fold_in(arg_keys[7], 71), 0)
    w_patch = centred(arg_keys[1], (PATCH_IN, D), PATCH_IN ** -0.5, 0.21875)
    patch_bias = centred(arg_keys[2], (D,), 1.0, 5.0)
    ln_gain = jnp.clip(1.0 + 0.1 * jax.random.normal(arg_keys[3], (D,), jnp.float32), 0.5, 1.5).astype(jnp.bfloat16)
    w_qkv = draw_w_qkv(jax.random.fold_in(arg_keys[7], 71), 0)
    qk_gain = draw_qk_gain(jax.random.fold_in(arg_keys[7], 71), 0)
    w_out = centred(arg_keys[6], (H, HD, D), (H * HD) ** -0.5, 0.078125, ((0, 8), (2, 4)))
    return dict(patches=patches, w_patch=w_patch, patch_bias=patch_bias, ln_gain=ln_gain, w_qkv=w_qkv, qk_gain=qk_gain, w_out=w_out)


NORM_EPS = 1e-06

def sincos_table(row_ids, col_ids, model_width):
    quarter = model_width // 4
    frequency = 1.0 / 10000.0 ** (jnp.arange(quarter, dtype=jnp.float32) / quarter)
    row_angle = row_ids.astype(jnp.float32)[:, None] * frequency[None, :]
    col_angle = col_ids.astype(jnp.float32)[:, None] * frequency[None, :]
    return jnp.concatenate([jnp.sin(row_angle), jnp.cos(row_angle), jnp.sin(col_angle), jnp.cos(col_angle)], axis=1)

def layer_norm(values, gain_row):
    mean_val = lax.optimization_barrier(jnp.mean(values, axis=-1, keepdims=True))
    centered = values - mean_val
    variance = lax.optimization_barrier(jnp.mean(centered * centered, axis=-1, keepdims=True))
    return centered * lax.rsqrt(variance + NORM_EPS) * gain_row

def reference(patches, w_patch, patch_bias, ln_gain, w_qkv, qk_gain, w_out):
    token_count = GH * GW
    token_ids = jnp.arange(token_count, dtype=jnp.int32)
    flat_pixels = patches.reshape(token_count, PATCH_IN)
    embedded = jnp.dot(flat_pixels, w_patch, preferred_element_type=jnp.float32)
    embedded = embedded + patch_bias.astype(jnp.float32)[None, :] + sincos_table(token_ids // GW, token_ids % GW, D)
    normed = layer_norm(embedded, ln_gain.astype(jnp.float32)).astype(jnp.bfloat16)
    projected = jnp.dot(normed, w_qkv.reshape(D, 3 * H * HD), preferred_element_type=jnp.float32)
    projected = projected.reshape(token_count, 3, H, HD)
    queries = layer_norm(projected[:, 0], qk_gain[0]).astype(jnp.bfloat16)
    keys_all = layer_norm(projected[:, 1], qk_gain[1]).astype(jnp.bfloat16)
    values_all = projected[:, 2].astype(jnp.bfloat16)
    scale_factor = 1.0 / math.sqrt(HD)
    query_block = math.gcd(token_count, 1024)

    def one_head(head_args):
        head_q, head_k, head_v = head_args

        def one_block(block_q):
            scores = jnp.dot(block_q, head_k.T, preferred_element_type=jnp.float32) * scale_factor
            row_peak = lax.optimization_barrier(jnp.max(scores, axis=1, keepdims=True))
            exponent = jnp.exp(scores - row_peak)
            weight_sum = lax.optimization_barrier(jnp.sum(exponent, axis=1, keepdims=True))
            mixed_sum = jnp.dot(exponent.astype(jnp.bfloat16), head_v, preferred_element_type=jnp.float32)
            return (mixed_sum / weight_sum).astype(jnp.bfloat16)
        blocks = lax.map(one_block, head_q.reshape(token_count // query_block, query_block, HD))
        return blocks.reshape(token_count, HD)
    context = lax.map(one_head, (queries.transpose(1, 0, 2), keys_all.transpose(1, 0, 2), values_all.transpose(1, 0, 2)))
    context = context.transpose(1, 0, 2).reshape(token_count, H * HD)
    grouped_ctx = context.reshape(token_count, N_COL, H // N_COL * HD).transpose(1, 0, 2)
    grouped_w = w_out.reshape(N_COL, H // N_COL * HD, D)

    def add_group(running, group_args):
        group_ctx, group_w = group_args
        partial_term = jnp.dot(group_ctx, group_w, preferred_element_type=jnp.float32)
        rounded = lax.optimization_barrier(partial_term.astype(jnp.bfloat16))
        return (running + rounded.astype(jnp.float32), None)
    summed, unused = lax.scan(add_group, jnp.zeros((token_count, D), jnp.float32), (grouped_ctx, grouped_w))
    return summed.astype(jnp.bfloat16)
```

```python
import functools
import math

import jax
import jax.numpy as jnp
from jax import lax
from jax.experimental import pallas as pl
from jax.experimental.pallas import tpu as pltpu
from jax.sharding import PartitionSpec as P

NORM_EPS = 1e-06
KEY_BLOCK = 1024
CHUNKS = 4
MISC = 16
F32 = jnp.float32
BF16 = jnp.bfloat16


def sincos_half(ids, model_width):
    quarter = model_width // 4
    frequency = 1.0 / 10000.0 ** (jnp.arange(quarter, dtype=jnp.float32) / quarter)
    angle = ids.astype(jnp.float32)[:, None] * frequency[None, :]
    return jnp.concatenate([jnp.sin(angle), jnp.cos(angle)], axis=1)


def fold_kernel(group, centred_steps, depth, wp_ref, gain_ref, bias_ref, table_ref, tmean_ref,
                w_ref, f_ref, r_ref, c_ref, a_ref, acc_ref, row_acc):
    step = pl.program_id(0)
    pix, width = wp_ref.shape
    half = width // 2
    grid_rows, grid_cols = r_ref.shape[0], c_ref.shape[0]
    positions = table_ref.shape[0]
    base = pix + MISC

    @pl.when(step == 0)
    def _():
        gain = gain_ref[...]

        def centre(i, carry):
            rows = pl.ds(pl.multiple_of(i * 16, 16), 16)
            w = wp_ref[rows, :].astype(F32)
            mean = jnp.mean(w, axis=1, keepdims=True)
            a_ref[rows, :] = ((w - mean) * gain).astype(BF16)
            return carry

        lax.fori_loop(0, pix // 16, centre, 0)
        bias = bias_ref[...]
        bias = (bias - jnp.mean(bias, axis=1, keepdims=True)) * gain
        high = bias.astype(BF16).astype(F32)
        row = lax.broadcasted_iota(jnp.int32, (MISC, 1), 0)
        misc = jnp.where(row == 0, high, 0.0) + jnp.where(row == 1, bias - high, 0.0)
        a_ref[pix:base, :] = (misc + jnp.where(row == 2, gain, 0.0)).astype(BF16)

        def place(i, carry):
            rows = pl.ds(pl.multiple_of(i * 16, 16), 16)
            to = pl.ds(pl.multiple_of(base + i * 16, 16), 16)
            t = table_ref[rows, :]
            a_ref[to, :half] = (t * gain[:, :half]).astype(BF16)
            a_ref[to, half:] = (t * gain[:, half:]).astype(BF16)
            return carry

        lax.fori_loop(0, positions // 16, place, 0)

    def add(i, carry):
        ks = pl.ds(pl.multiple_of(i * depth, depth), depth)
        w = jnp.concatenate([w_ref[g, ks, :] for g in range(group)], axis=1)
        acc_ref[...] += jnp.dot(a_ref[:, ks], w, preferred_element_type=F32)
        return carry

    acc_ref[...] = jnp.zeros_like(acc_ref)
    lax.fori_loop(0, half // depth, add, 0)
    row_acc[...] = acc_ref[base : base + grid_rows, :]
    acc_ref[base:, :] = jnp.zeros((positions, acc_ref.shape[1]), F32)
    lax.fori_loop(half // depth, width // depth, add, 0)
    bias_w = acc_ref[pix : pix + 1, :] + acc_ref[pix + 1 : pix + 2, :]
    gain_w = acc_ref[pix + 2 : pix + 3, :]
    r = row_acc[...] - tmean_ref[:grid_rows, :] * gain_w
    c = acc_ref[base : base + grid_cols, :] - tmean_ref[:grid_cols, :] * gain_w + bias_w
    f = acc_ref[:pix, :]
    size = f.shape[1] // group
    keep = jnp.where(step < centred_steps, 1.0, 0.0).astype(F32)
    for g in range(group):
        at = slice(g * size, (g + 1) * size)
        for value, out in ((f, f_ref), (r, r_ref), (c, c_ref)):
            part = value[:, at]
            part = part - keep * jnp.mean(part, axis=1, keepdims=True)
            out[:, at] = part.astype(out.dtype)


def fold(w_patch, gain, bias, table, heads_w, heads_here, grid_rows, grid_cols):
    pix, width = w_patch.shape
    total, _, size = heads_w.shape
    group = next(g for g in (2, 3, 1) if heads_here % g == 0)
    steps = total // group
    positions = table.shape[0]
    rows = pix + MISC + positions
    depth = math.gcd(width // 2, 1024)
    tmean = jnp.sum(table, axis=1, keepdims=True) / width
    whole = lambda s: pl.BlockSpec(s, lambda i: (0,) * len(s), pipeline_mode=pl.Buffered(1))
    return pl.pallas_call(
        functools.partial(fold_kernel, group, 2 * heads_here // group, depth),
        grid=(steps,),
        in_specs=[
            whole((pix, width)),
            whole((1, width)),
            whole((1, width)),
            whole(table.shape),
            whole((positions, 1)),
            pl.BlockSpec((group, width, size), lambda i: (i, 0, 0)),
        ],
        out_specs=[
            pl.BlockSpec((pix, group * size), lambda i: (0, i)),
            pl.BlockSpec((grid_rows, group * size), lambda i: (0, i)),
            pl.BlockSpec((grid_cols, group * size), lambda i: (0, i)),
        ],
        out_shape=[
            jax.ShapeDtypeStruct((pix, total * size), BF16),
            jax.ShapeDtypeStruct((grid_rows, total * size), F32),
            jax.ShapeDtypeStruct((grid_cols, total * size), F32),
        ],
        scratch_shapes=[
            pltpu.VMEM((rows, width), BF16),
            pltpu.VMEM((rows, group * size), F32),
            pltpu.VMEM((grid_rows, group * size), F32),
        ],
        compiler_params=pltpu.CompilerParams(
            dimension_semantics=("arbitrary",), vmem_limit_bytes=56 * 1024 * 1024
        ),
        cost_estimate=pl.CostEstimate(
            flops=2 * rows * width * total * size,
            bytes_accessed=2 * width * total * size,
            transcendentals=0,
        ),
        name="fold",
    )(w_patch, gain, bias, table, tmean, heads_w)


def project_kernel(size, normed_width, p_ref, f_ref, r_ref, c_ref, gain_ref, rstd_ref, out_ref):
    lines = r_ref.shape[0]
    cols = c_ref.shape[0]
    width = f_ref.shape[1]
    chunk = 2 * size if width % (2 * size) == 0 and normed_width % (2 * size) == 0 else size
    for line in range(lines):
        rows = slice(line * cols, (line + 1) * cols)
        rstd = rstd_ref[rows, :]
        for start in range(0, width, chunk):
            x = jnp.dot(p_ref[rows, :], f_ref[:, start : start + chunk], preferred_element_type=F32)
            x = x + (c_ref[:, start : start + chunk] + r_ref[line : line + 1, start : start + chunk])
            for at in range(0, chunk, size):
                part = x[:, at : at + size]
                to = slice(start + at, start + at + size)
                if start + at < normed_width:
                    square = jnp.sum(part * part, axis=1, keepdims=True) * (1.0 / size)
                    scale = rstd * lax.rsqrt(square * rstd * rstd + NORM_EPS)
                    part = part * scale * gain_ref[:, to]
                else:
                    part = part * rstd
                out_ref[rows, to] = part.astype(out_ref.dtype)


def project(pixels, f, r, c, gain, rstd, first, width, size, lines):
    tokens, pix = pixels.shape
    cols = c.shape[0]
    at = first // width
    normed_width = gain.shape[1]
    return pl.pallas_call(
        functools.partial(project_kernel, size, normed_width),
        grid=(tokens // (lines * cols),),
        in_specs=[
            pl.BlockSpec((lines * cols, pix), lambda i: (i, 0)),
            pl.BlockSpec((pix, width), lambda i: (0, 0)),
            pl.BlockSpec((lines, width), lambda i: (i, 0)),
            pl.BlockSpec((cols, width), lambda i: (0, 0)),
            pl.BlockSpec((1, normed_width), lambda i: (0, 0)),
            pl.BlockSpec((lines * cols, 1), lambda i: (i, 0)),
        ],
        out_specs=pl.BlockSpec((lines * cols, width), lambda i: (i, 0)),
        out_shape=jax.ShapeDtypeStruct((tokens, width), BF16),
        compiler_params=pltpu.CompilerParams(
            dimension_semantics=("arbitrary",), vmem_limit_bytes=48 * 1024 * 1024
        ),
        cost_estimate=pl.CostEstimate(
            flops=2 * tokens * pix * width, bytes_accessed=4 * tokens * width, transcendentals=tokens
        ),
        name="project",
    )(pixels, f, r, c, gain, rstd)


def attention_kernel(key_block, q_ref, k_ref, v_ref, out_ref):
    rows, head_size = math.prod(q_ref.shape[:-1]), q_ref.shape[-1]
    query = q_ref[...].reshape(rows, head_size)
    peak = jnp.full((rows, 1), -1e30, F32)
    total = jnp.zeros((rows, 1), F32)
    acc = jnp.zeros((rows, head_size), F32)
    for start in range(0, k_ref.shape[0], key_block):
        scores = lax.dot_general(
            query,
            k_ref[start : start + key_block, :],
            (((1,), (1,)), ((), ())),
            preferred_element_type=F32,
        )
        new_peak = jnp.maximum(peak, jnp.max(scores, axis=1, keepdims=True))
        rescale = jnp.exp2(peak - new_peak)
        weights = jnp.exp2(scores - new_peak)
        total = total * rescale + jnp.sum(weights, axis=1, keepdims=True)
        acc = acc * rescale + jnp.dot(
            weights.astype(BF16), v_ref[start : start + key_block, :], preferred_element_type=F32
        )
        peak = new_peak
    out_ref[...] = (acc / total).astype(out_ref.dtype).reshape(out_ref.shape)


def attention(queries, keys_values, chunk, chunk_rows, width, head_size):
    owners = queries.shape[0]
    heads = width // head_size
    key_count = keys_values.shape[0]
    key_block = math.gcd(key_count, KEY_BLOCK)
    rows = owners * chunk_rows
    elements = heads * rows * key_count
    return pl.pallas_call(
        functools.partial(attention_kernel, key_block),
        grid=(heads,),
        in_specs=[
            pl.BlockSpec((owners, chunk_rows, head_size), lambda h: (0, chunk, h)),
            pl.BlockSpec((key_count, head_size), lambda h: (0, h)),
            pl.BlockSpec((key_count, head_size), lambda h: (0, heads + h)),
        ],
        out_specs=pl.BlockSpec((owners, chunk_rows, head_size), lambda h: (0, 0, h)),
        out_shape=jax.ShapeDtypeStruct((owners, chunk_rows, width), BF16),
        compiler_params=pltpu.CompilerParams(
            dimension_semantics=("arbitrary",), vmem_limit_bytes=48 * 1024 * 1024
        ),
        cost_estimate=pl.CostEstimate(
            flops=4 * elements * head_size,
            bytes_accessed=4 * (rows + key_count) * width,
            transcendentals=elements,
        ),
        name="attention",
    )(queries, keys_values, keys_values)


def local(patches, w_patch, patch_bias, ln_gain, w_qkv, qk_gain, w_out):
    tile_rows, tile_cols, pix = patches.shape
    model_width = w_patch.shape[1]
    heads_here, size = w_qkv.shape[2], w_qkv.shape[3]
    head_width = heads_here * size
    col_count, row_count = lax.axis_size("col"), lax.axis_size("row")
    grid_rows, grid_cols = tile_rows * row_count, tile_cols * col_count
    block_tokens = tile_rows * grid_cols
    row_anchor = lax.axis_index("row") * tile_rows
    col_anchor = lax.axis_index("col") * tile_cols

    pixels = lax.all_gather(patches, "col", axis=1, tiled=True)
    pixels = lax.all_gather(pixels, "row", axis=0, tiled=True).reshape(-1, pix)
    out_weight = lax.all_gather(w_out, "row", axis=2, tiled=True).reshape(head_width, model_width)

    bias = patch_bias.astype(F32)[None, :]
    gain = ln_gain.astype(F32)[None, :]
    positions = max(grid_rows, grid_cols)
    table = sincos_half(jnp.arange(positions, dtype=jnp.int32), model_width)
    table = lax.optimization_barrier(table)

    shape = (tile_rows, tile_cols, model_width // 2)
    row_half = lax.dynamic_slice_in_dim(table, row_anchor, tile_rows)
    col_half = lax.dynamic_slice_in_dim(table, col_anchor, tile_cols)
    position = jnp.concatenate(
        [jnp.broadcast_to(row_half[:, None], shape), jnp.broadcast_to(col_half[None], shape)], axis=2
    ).reshape(tile_rows * tile_cols, model_width)
    embedded = jnp.dot(patches.reshape(-1, pix), w_patch, preferred_element_type=F32)
    embedded = embedded + bias + position
    centred = embedded - jnp.mean(embedded, axis=1, keepdims=True)
    variance = jnp.mean(centred * centred, axis=1)
    rstd = lax.rsqrt(variance + NORM_EPS).reshape(tile_rows, tile_cols)
    rstd = lax.all_gather(rstd, "col", axis=1, tiled=True)
    rstd = lax.all_gather(rstd, "row", axis=0, tiled=True).reshape(-1, 1)

    heads_w = w_qkv.transpose(1, 2, 0, 3).reshape(3 * heads_here, model_width, size)
    f, r, c = fold(w_patch, gain, bias, table, heads_w, heads_here, grid_rows, grid_cols)

    q_gain = qk_gain[0].reshape(1, head_width) * (math.log2(math.e) / math.sqrt(size))
    k_gain = qk_gain[1].reshape(1, head_width)
    lines = tile_rows
    keys_values = project(
        pixels, f[:, head_width:], r[:, head_width:], c[:, head_width:], k_gain, rstd, 0,
        2 * head_width, size, lines
    )
    own = row_anchor * grid_cols
    queries = project(
        lax.dynamic_slice_in_dim(pixels, own, block_tokens),
        f[:, :head_width],
        lax.dynamic_slice_in_dim(r[:, :head_width], row_anchor, tile_rows),
        c[:, :head_width], q_gain,
        lax.dynamic_slice_in_dim(rstd, own, block_tokens), 0, head_width, size, lines
    )
    owned = block_tokens // col_count
    chunk_rows = owned // math.gcd(owned // 16, CHUNKS)
    queries = queries.reshape(col_count, owned, head_width)
    pieces = []
    for chunk in range(owned // chunk_rows):
        context = attention(queries, keys_values, chunk, chunk_rows, head_width, size)
        partial = jnp.dot(
            context.reshape(col_count * chunk_rows, head_width), out_weight,
            preferred_element_type=F32,
        ).astype(BF16)
        pieces.append(lax.psum_scatter(partial, "col", scatter_dimension=0, tiled=True))
    return jnp.concatenate(pieces, axis=0)


def solution(mesh):
    return jax.shard_map(
        local,
        mesh=mesh,
        in_specs=(
            P("row", "col", None),
            P(),
            P(),
            P(),
            P(None, None, "col", None),
            P(None, "col", None),
            P("col", None, "row"),
        ),
        out_specs=P(("row", "col"), None),
        check_vma=False,
    )
```

```python
import functools
import math

import jax
import jax.numpy as jnp
from jax import lax
from jax.experimental import pallas as pl
from jax.experimental.pallas import tpu as pltpu
from jax.sharding import PartitionSpec as P

NORM_EPS = 1e-06
KEY_BLOCK = 1024
CHUNKS = 4
MISC = 16
F32 = jnp.float32
BF16 = jnp.bfloat16


def sincos_half(ids, model_width):
    quarter = model_width // 4
    frequency = 1.0 / 10000.0 ** (jnp.arange(quarter, dtype=jnp.float32) / quarter)
    angle = ids.astype(jnp.float32)[:, None] * frequency[None, :]
    return jnp.concatenate([jnp.sin(angle), jnp.cos(angle)], axis=1)


def ids():
    row, col = lax.axis_index("row"), lax.axis_index("col")
    return row, col, lax.div(col, 2), lax.rem(col, 2)


def row_peer(row, hop, count):
    if count != 4:
        return lax.rem(row + hop, count)
    if hop == 1:
        return row + 1 - 2 * lax.rem(row, 2)
    if hop == 2:
        return lax.rem(row + 2, 4)
    return 3 - row


def remote(src, dst, send, recv, row, col):
    return pltpu.make_async_remote_copy(
        src_ref=src, dst_ref=dst, send_sem=send, recv_sem=recv,
        device_id=(row, col), device_id_type=pl.DeviceIdType.MESH,
    )


def prep_kernel(sizes, group, centred_steps, patch_ref, wp_ref, gain_ref, bias_ref, table_ref,
                tmean_ref, w_ref, f_ref, r_ref, c_ref, pixels_ref, rstd_ref,
                a_ref, acc_ref, row_acc, e_ref, mine_ref, seen_ref,
                local_sem, send_sem, recv_sem, stat_send, stat_recv):
    row_count, col_count, tile_rows, tile_cols = sizes
    step = pl.program_id(0)
    last = pl.num_programs(0) - 1
    pix, width = wp_ref.shape
    half = width // 2
    grid_rows, grid_cols = r_ref.shape[0], c_ref.shape[0]
    positions = table_ref.shape[0]
    base = pix + MISC
    tokens = tile_rows * tile_cols
    row, col, line, core = ids()
    me = row * col_count + col
    devices = row_count * col_count
    lines = col_count // 2
    partner = 2 * line + 1 - core

    def give(src, block, to_row, to_col):
        remote(src, pixels_ref.at[block], send_sem, recv_sem.at[block], to_row, to_col).start()

    def got(block):
        pltpu.make_async_copy(pixels_ref.at[block], pixels_ref.at[block], recv_sem.at[block]).wait()

    def to_rows(src, block):
        for hop in range(1, row_count):
            give(src, block, row_peer(row, hop, row_count), col)

    @pl.when(step == 0)
    def _():
        for hop in range(1, lines):
            give(patch_ref, me, row, 2 * lax.rem(line + hop, lines) + core)
        to_rows(patch_ref, me)
        give(patch_ref, me, row, partner)
        pltpu.make_async_copy(patch_ref, pixels_ref.at[me], local_sem).start()
        gain = gain_ref[...]

        def centre(i, carry):
            rows = pl.ds(pl.multiple_of(i * 16, 16), 16)
            w = wp_ref[rows, :].astype(F32)
            mean = jnp.sum(w, axis=1, keepdims=True) * (1.0 / width)
            a_ref[rows, :] = ((w - mean) * gain).astype(BF16)
            return carry

        lax.fori_loop(0, pix // 16, centre, 0)
        bias = bias_ref[...]
        bias = (bias - jnp.mean(bias, axis=1, keepdims=True)) * gain
        high = bias.astype(BF16).astype(F32)
        at = lax.broadcasted_iota(jnp.int32, (MISC, 1), 0)
        misc = jnp.where(at == 0, high, 0.0) + jnp.where(at == 1, bias - high, 0.0)
        a_ref[pix:base, :] = (misc + jnp.where(at == 2, gain, 0.0)).astype(BF16)

        def place(i, carry):
            rows = pl.ds(pl.multiple_of(i * 16, 16), 16)
            to = pl.ds(pl.multiple_of(base + i * 16, 16), 16)
            t = table_ref[rows, :]
            a_ref[to, :half] = (t * gain[:, :half]).astype(BF16)
            a_ref[to, half:] = (t * gain[:, half:]).astype(BF16)
            return carry

        lax.fori_loop(0, positions // 16, place, 0)

    @pl.when(step == 1)
    def _():
        chunk = math.gcd(half, 512)
        own_rows = pl.ds(pl.multiple_of(row * tile_rows, 8), tile_rows)
        own_cols = pl.ds(pl.multiple_of(col * tile_cols, 8), tile_cols)
        shape = (tile_rows, tile_cols, chunk)

        def embed(i, carry):
            for side in range(2):
                at = pl.ds(pl.multiple_of(i * chunk, chunk), chunk)
                to = pl.ds(pl.multiple_of(side * half + i * chunk, chunk), chunk)
                if side == 0:
                    t = jnp.broadcast_to(table_ref[own_rows, at][:, None, :], shape)
                else:
                    t = jnp.broadcast_to(table_ref[own_cols, at][None, :, :], shape)
                e = jnp.dot(patch_ref[...], wp_ref[:, to], preferred_element_type=F32)
                e_ref[:, to] = e + bias_ref[:, to] + t.reshape(tokens, chunk)
            return carry

        lax.fori_loop(0, half // chunk, embed, 0)
        mean = jnp.sum(e_ref[...], axis=1, keepdims=True) * (1.0 / width)
        centred = e_ref[...] - mean
        variance = jnp.sum(centred * centred, axis=1, keepdims=True) * (1.0 / width)
        rstd = jnp.broadcast_to(lax.rsqrt(variance + NORM_EPS), (tokens, 128))
        mine_ref[...] = rstd.T[:8, :]

        def tell(hop, carry):
            to = lax.rem(me + hop, devices)
            remote(mine_ref, seen_ref.at[hop - 1], stat_send, stat_recv,
                   lax.div(to, col_count), lax.rem(to, col_count)).start()
            return carry

        lax.fori_loop(1, devices, tell, 0)
        seen_ref[devices - 1] = mine_ref[...]

    @pl.when(step == jnp.minimum(3, last))
    def _():
        for hop in range(1, lines):
            block = row * col_count + 2 * lax.rem(line + hop, lines) + core
            got(block)
            to_rows(pixels_ref.at[block], block)
            give(pixels_ref.at[block], block, row, partner)

    def product(start):
        ks = slice(start, start + half)
        w = jnp.concatenate([w_ref[g, ks, :] for g in range(group)], axis=1)
        return jnp.dot(a_ref[:, ks], w, preferred_element_type=F32)

    acc_ref[...] = product(0)
    row_acc[...] = acc_ref[base : base + grid_rows, :]
    acc_ref[base:, :] = jnp.zeros((positions, acc_ref.shape[1]), F32)
    acc_ref[...] += product(half)
    bias_w = acc_ref[pix : pix + 1, :] + acc_ref[pix + 1 : pix + 2, :]
    gain_w = acc_ref[pix + 2 : pix + 3, :]
    r = row_acc[...] - tmean_ref[:grid_rows, :] * gain_w
    c = acc_ref[base : base + grid_cols, :] - tmean_ref[:grid_cols, :] * gain_w + bias_w
    f = acc_ref[:pix, :]
    size = f.shape[1] // group
    keep = jnp.where(step < centred_steps, 1.0, 0.0).astype(F32)
    for g in range(group):
        at = slice(g * size, (g + 1) * size)
        for value, out in ((f, f_ref), (r, r_ref), (c, c_ref)):
            part = value[:, at]
            part = part - keep * jnp.mean(part, axis=1, keepdims=True)
            out[:, at] = part.astype(out.dtype)

    @pl.when(step == last)
    def _():
        for hop in range(1, row_count):
            for i in range(lines):
                block = row_peer(row, hop, row_count) * col_count + 2 * i + core
                got(block)
                give(pixels_ref.at[block], block, row, partner)
        for other in range(row_count):
            for i in range(lines):
                got(other * col_count + 2 * i + 1 - core)
        everyone = pixels_ref.at[pl.ds(0, devices - 1)]
        pltpu.make_async_copy(everyone, everyone, send_sem).wait()
        pltpu.make_async_copy(patch_ref, pixels_ref.at[me], local_sem).wait()
        seen = seen_ref.at[pl.ds(0, devices - 1)]
        pltpu.make_async_copy(seen, seen, stat_recv).wait()
        pltpu.make_async_copy(seen, seen, stat_send).wait()

        def put(block, carry):
            rstd_ref[block] = seen_ref[lax.rem(me - block + 2 * devices - 1, devices)]
            return carry

        lax.fori_loop(0, devices, put, 0)


def prep(patches, w_patch, gain, bias, table, heads_w, sizes, heads_here, grid_rows, grid_cols):
    pix, width = w_patch.shape
    total, _, size = heads_w.shape
    group = next(g for g in (2, 3, 1) if heads_here % g == 0)
    steps = total // group
    positions = table.shape[0]
    rows = pix + MISC + positions
    tokens = patches.shape[0]
    devices = sizes[0] * sizes[1]
    tmean = jnp.sum(table, axis=1, keepdims=True) / width
    whole = lambda s: pl.BlockSpec(s, lambda i: (0,) * len(s), pipeline_mode=pl.Buffered(1))
    return pl.pallas_call(
        functools.partial(prep_kernel, sizes, group, 2 * heads_here // group),
        grid=(steps,),
        in_specs=[
            whole((tokens, pix)),
            whole((pix, width)),
            whole((1, width)),
            whole((1, width)),
            whole(table.shape),
            whole((positions, 1)),
            pl.BlockSpec((group, width, size), lambda i: (i, 0, 0)),
        ],
        out_specs=[
            pl.BlockSpec((pix, group * size), lambda i: (0, i)),
            pl.BlockSpec((grid_rows, group * size), lambda i: (0, i)),
            pl.BlockSpec((grid_cols, group * size), lambda i: (0, i)),
            pl.BlockSpec(memory_space=pl.ANY),
            pl.BlockSpec((devices, 8, tokens), lambda i: (0, 0, 0)),
        ],
        out_shape=[
            jax.ShapeDtypeStruct((pix, total * size), BF16),
            jax.ShapeDtypeStruct((grid_rows, total * size), F32),
            jax.ShapeDtypeStruct((grid_cols, total * size), F32),
            jax.ShapeDtypeStruct((devices, tokens, pix), BF16),
            jax.ShapeDtypeStruct((devices, 8, tokens), F32),
        ],
        scratch_shapes=[
            pltpu.VMEM((rows, width), BF16),
            pltpu.VMEM((rows, group * size), F32),
            pltpu.VMEM((grid_rows, group * size), F32),
            pltpu.VMEM((tokens, width), F32),
            pltpu.VMEM((8, tokens), F32),
            pltpu.VMEM((devices, 8, tokens), F32),
            pltpu.SemaphoreType.DMA,
            pltpu.SemaphoreType.DMA,
            pltpu.SemaphoreType.DMA((devices,)),
            pltpu.SemaphoreType.DMA,
            pltpu.SemaphoreType.DMA,
        ],
        compiler_params=pltpu.CompilerParams(
            dimension_semantics=("arbitrary",), vmem_limit_bytes=60 * 1024 * 1024,
            has_side_effects=True,
        ),
        cost_estimate=pl.CostEstimate(
            flops=2 * rows * width * total * size,
            bytes_accessed=2 * width * total * size,
            transcendentals=0,
        ),
        name="prep",
    )(patches, w_patch, gain, bias, table, tmean, heads_w)

def attention_block(key_block, query, k_ref, v_ref):
    rows, head_size = query.shape
    peak = jnp.full((rows, 1), -1e30, F32)
    total = jnp.zeros((rows, 1), F32)
    acc = jnp.zeros((rows, head_size), F32)
    for start in range(0, k_ref.shape[0], key_block):
        scores = lax.dot_general(
            query,
            k_ref[start : start + key_block, :],
            (((1,), (1,)), ((), ())),
            preferred_element_type=F32,
        )
        new_peak = jnp.maximum(peak, jnp.max(scores, axis=1, keepdims=True))
        rescale = jnp.exp2(peak - new_peak)
        weights = jnp.exp2(scores - new_peak)
        total = total * rescale + jnp.sum(weights, axis=1, keepdims=True)
        acc = acc * rescale + jnp.dot(
            weights.astype(BF16), v_ref[start : start + key_block, :], preferred_element_type=F32
        )
        peak = new_peak
    return (acc / total).astype(BF16)


def attend_kernel(sizes, heads, key_block, pixels_ref, f_ref, r_ref, c_ref, gain_ref, rstd_ref,
                  rq_ref, w_ref, out_ref, kv_ref, wall_ref, pbuf_ref, qbuf_ref, q_ref, ctx_ref,
                  pair_ref, hop_ref, own_ref, stage_ref, w_local, w_send, w_recv, p_sem, q_sem,
                  stage_send, pair_recv, hop_send, hop_recv):
    row_count, col_count, tile_rows, tile_cols = sizes
    row, col, line, core = ids()
    lines = col_count // 2
    partner = 2 * line + 1 - core
    size = kv_ref.shape[2]
    head_width = heads * size
    blocks, tokens, pix = pbuf_ref.shape[1:]
    owned = tile_cols * tile_rows
    per_line = tile_cols * col_count // owned
    part = wall_ref.shape[2]
    wide = 2 * size
    is_end = jnp.logical_or(line == 0, line == lines - 1)

    def wait(ref, sem):
        pltpu.make_async_copy(ref, ref, sem).wait()

    def order(s):
        up = jnp.where(s < lines - 1 - line, lines - 1 - s, s - (lines - 1 - line))
        down = jnp.where(s < line, s, lines - 1 - (s - line))
        far = jnp.where(2 * line < lines, up, down)
        return jnp.where(s == lines - 1, line, far)

    relay = row_count == 4
    piece = part // 2

    def relayed(side):
        at = pl.ds(side * piece, piece)
        return remote(wall_ref.at[1 + side, :, at], wall_ref.at[3, :, at], w_send.at[3 + side],
                      w_recv.at[3 + side], row_peer(row, 2 - side, row_count), col)

    for hop in range(1, 3 if relay else row_count):
        remote(w_ref, wall_ref.at[hop], w_send.at[hop], w_recv.at[hop],
               row_peer(row, hop, row_count), col).start()
    pltpu.make_async_copy(w_ref, wall_ref.at[0], w_local).start()

    def fetch(i):
        slot = lax.rem(i, 2)
        return pltpu.make_async_copy(
            pixels_ref.at[pl.ds(i * blocks, blocks)], pbuf_ref.at[slot], p_sem.at[slot]
        )

    def q_row(s, side):
        return 2 * order(s) + (core if side else 1 - core)

    def fetch_q(s):
        for side in range(2):
            mine = q_row(s, side)
            first = lax.rem(mine, per_line) * tile_rows
            lane = pl.multiple_of(lax.div(mine, per_line) * tile_cols, tile_cols)
            for c in range(tile_rows):
                pltpu.make_async_copy(
                    pixels_ref.at[row * col_count + first + c, pl.ds(lane, tile_cols), :],
                    qbuf_ref.at[pl.ds(side * owned + c * tile_cols, tile_cols), :],
                    q_sem,
                ).start()

    def pick(rows, index):
        at = lax.broadcasted_iota(jnp.int32, rows.shape, 0)
        return jnp.sum(jnp.where(at == index, rows, 0.0), axis=0, keepdims=True)

    def normed(x, scale_rows, gain):
        square = jnp.sum(x * x, axis=1, keepdims=True) * (1.0 / size)
        return x * (scale_rows * lax.rsqrt(square * scale_rows * scale_rows + NORM_EPS)) * gain

    fetch(0).start()
    fetch_q(0)
    rounds = pixels_ref.shape[0] // blocks

    def keys_values(i, carry):
        fetch(i).wait()

        @pl.when(i + 1 < rounds)
        def _():
            fetch(i + 1).start()

        p = pbuf_ref[lax.rem(i, 2)].reshape(blocks * tokens, pix)
        rstd = []
        for b in range(blocks):
            lanes = rstd_ref[i * blocks + b][0:1, :]
            rstd.append(jnp.broadcast_to(lanes, (size, tokens)).T)
        for start in range(0, 2 * head_width, wide):
            at = slice(head_width + start, head_width + start + wide)
            x = jnp.dot(p, f_ref[:, at], preferred_element_type=F32)
            for b in range(blocks):
                block = i * blocks + b
                rows = pl.ds(pl.multiple_of(lax.div(block, col_count) * tile_rows, 8), tile_rows)
                cols = pl.ds(pl.multiple_of(lax.rem(block, col_count) * tile_cols, 8), tile_cols)
                u = c_ref[cols, at][None, :, :] + r_ref[rows, at][:, None, :]
                y = x[b * tokens : (b + 1) * tokens] + u.reshape(tokens, wide)
                to = pl.ds(pl.multiple_of(block * tokens, tokens), tokens)
                for g in range(2):
                    head = start // size + g
                    z = y[:, g * size : (g + 1) * size]
                    if head < heads:
                        gain = gain_ref[:, head_width + head * size : head_width + (head + 1) * size]
                        z = normed(z, rstd[b], gain)
                    else:
                        z = z * rstd[b]
                    kv_ref[head, to, :] = z.astype(BF16)
        return carry

    lax.fori_loop(0, rounds, keys_values, 0)

    def attend(s):
        wait(qbuf_ref, q_sem)
        for start in range(0, head_width, size):
            at = slice(start, start + size)
            x = jnp.dot(qbuf_ref[...], f_ref[:, at], preferred_element_type=F32)
            for side in range(2):
                mine = q_row(s, side)
                cols = pl.ds(pl.multiple_of(lax.rem(mine, per_line) * owned, owned), owned)
                own_rows = pl.ds(pl.multiple_of(row * tile_rows, 8), tile_rows)
                u = c_ref[cols, at] + pick(r_ref[own_rows, at], lax.div(mine, per_line))
                rstd = jnp.broadcast_to(pick(rq_ref[...], mine), (size, owned)).T
                y = normed(x[side * owned : (side + 1) * owned] + u, rstd, gain_ref[:, at])
                q_ref[start // size, side * owned : (side + 1) * owned, :] = y.astype(BF16)

        @pl.when(s + 1 < lines)
        def _():
            fetch_q(s + 1)

        def one_head(h, carry):
            to = pl.ds(pl.multiple_of(h * size, size), size)
            ctx_ref[s, :, to] = attention_block(
                key_block, q_ref[h], kv_ref.at[h], kv_ref.at[heads + h]
            )
            return carry

        lax.fori_loop(0, heads, one_head, 0)

    chunk = math.gcd(part, 512)

    def project_out(n, s, j):
        slot = lax.rem(n, 2)
        dest = order(s)

        @pl.when(n >= 2)
        def _():
            wait(stage_ref.at[slot], stage_send.at[slot])

        def columns(i, carry):
            at = pl.ds(pl.multiple_of(i * chunk, chunk), chunk)
            x = jnp.dot(ctx_ref[s], wall_ref[j, :, at], preferred_element_type=F32).astype(BF16)
            stage_ref[slot, :, at] = x[:owned]
            own_ref[:, at] = x[owned:]
            return carry

        lax.fori_loop(0, part // chunk, columns, 0)
        remote(stage_ref.at[slot], pair_ref.at[dest, j], stage_send.at[slot],
               pair_recv.at[dest, j], row, partner).start()
        wait(pair_ref.at[dest, j], pair_recv.at[dest, j])
        pair_ref[dest, j] = (pair_ref[dest, j].astype(F32) + own_ref[...].astype(F32)).astype(BF16)

    def pass_on(s, j):
        dest = order(s)
        up = dest > line
        to = jnp.where(up, line + 1, line - 1)
        slot = jnp.where(jnp.logical_and(dest == to, jnp.logical_not(up)), lines, dest)

        @pl.when(jnp.logical_not(is_end))
        def _():
            wait(hop_ref.at[dest, j], hop_recv.at[dest, j])
            total = pair_ref[dest, j].astype(F32) + hop_ref[dest, j].astype(F32)
            pair_ref[dest, j] = total.astype(BF16)

        remote(pair_ref.at[dest, j], hop_ref.at[slot, j], hop_send.at[dest, j],
               hop_recv.at[slot, j], row, 2 * to + core).start()

    inner = row_count - 2

    def group_size(s):
        return jnp.where(s == 0, 1, jnp.where(s == 1, 1 + 2 * inner, 1 + inner))

    def member(s, t):
        u = t - 1
        early = jnp.logical_and(s == 1, t > 0)
        return (jnp.where(early, lax.div(u, inner), s),
                jnp.where(early, 1 + lax.rem(u, inner), t))

    def group_start(s):
        return jnp.where(s < 2, s, 2 + 2 * inner + (s - 2) * (1 + inner))

    def step(s, carry):
        attend(s)

        @pl.when(s == 1)
        def _():
            for hop in range(1, row_count - 1):
                wait(wall_ref.at[hop], w_recv.at[hop])
            if relay:
                for side in range(2):
                    relayed(side).start()

        def make(t, c):
            ss, j = member(s, t)
            project_out(group_start(s) + t, ss, j)

            @pl.when(jnp.logical_and(is_end, ss < lines - 1))
            def _():
                pass_on(ss, j)

            return c

        lax.fori_loop(0, group_size(s), make, 0)

        @pl.when(jnp.logical_and(s > 0, jnp.logical_not(is_end)))
        def _():
            def late(t, c):
                pass_on(*member(s - 1, t))
                return c

            lax.fori_loop(0, group_size(s - 1), late, 0)

        return carry

    pltpu.make_async_copy(w_ref, wall_ref.at[0], w_local).wait()
    lax.fori_loop(0, lines, step, 0)
    final = row_count - 1
    if relay:
        for side in range(2):
            relayed(side).wait_recv()
    else:
        wait(wall_ref.at[final], w_recv.at[final])

    def make_last(s, c):
        project_out(group_start(lines) + s, s, final)

        @pl.when(jnp.logical_and(is_end, s < lines - 1))
        def _():
            pass_on(s, final)

        return c

    lax.fori_loop(0, lines, make_last, 0)

    def finish(j, sender):
        to = pl.ds(pl.multiple_of(sender * part, 128), part)
        side = jnp.where(line > 0, line, lines)
        wait(hop_ref.at[side, j], hop_recv.at[side, j])

        @pl.when(is_end)
        def _():
            total = pair_ref[line, j].astype(F32) + hop_ref[side, j].astype(F32)
            out_ref[:, to] = total.astype(BF16)

        @pl.when(jnp.logical_not(is_end))
        def _():
            wait(hop_ref.at[lines, j], hop_recv.at[lines, j])
            total = pair_ref[line, j].astype(F32) + hop_ref[line, j].astype(F32)
            out_ref[:, to] = (total + hop_ref[lines, j].astype(F32)).astype(BF16)

    def sender_of(hop):
        if hop == 0:
            return row
        if row_count == 4:
            return row_peer(row, hop, row_count)
        return lax.rem(row + row_count - hop, row_count)

    for j in range(row_count - 1):
        finish(j, sender_of(j))

    @pl.when(jnp.logical_not(is_end))
    def _():
        def late(s, c):
            pass_on(s, final)
            return c

        lax.fori_loop(0, lines - 1, late, 0)

    finish(final, sender_of(final))
    for hop in range(1, 3 if relay else row_count):
        wait(w_ref, w_send.at[hop])
    if relay:
        for side in range(2):
            relayed(side).wait_send()
    for slot in range(2):
        wait(stage_ref.at[slot], stage_send.at[slot])

    def drain(s, c):
        for j in range(row_count):
            wait(pair_ref.at[order(s), j], hop_send.at[order(s), j])
        return c

    lax.fori_loop(0, lines - 1, drain, 0)


def attend(pixels, f, r, c, gain, rstd, rq, w_out, sizes, heads, size):
    row_count, col_count, tile_rows, tile_cols = sizes
    devices, tokens, pix = pixels.shape
    head_width, part = w_out.shape
    lines = col_count // 2
    owned = tile_cols * tile_rows
    count = devices * tokens
    blocks = math.gcd(devices, 4)
    vmem = lambda: pl.BlockSpec(memory_space=pltpu.VMEM)
    hbm = lambda: pl.BlockSpec(memory_space=pl.ANY)
    dma = pltpu.SemaphoreType.DMA
    return pl.pallas_call(
        functools.partial(attend_kernel, sizes, heads, math.gcd(count, KEY_BLOCK)),
        in_specs=[hbm(), vmem(), vmem(), vmem(), vmem(), vmem(), vmem(), hbm()],
        out_specs=vmem(),
        out_shape=jax.ShapeDtypeStruct((owned, part * row_count), BF16),
        scratch_shapes=[
            pltpu.VMEM((2 * heads, count, size), BF16),
            pltpu.VMEM((row_count, head_width, part), BF16),
            pltpu.VMEM((2, blocks, tokens, pix), BF16),
            pltpu.VMEM((2 * owned, pix), BF16),
            pltpu.VMEM((heads, 2 * owned, size), BF16),
            pltpu.VMEM((lines, 2 * owned, head_width), BF16),
            pltpu.VMEM((lines, row_count, owned, part), BF16),
            pltpu.VMEM((lines + 1, row_count, owned, part), BF16),
            pltpu.VMEM((owned, part), BF16),
            pltpu.VMEM((2, owned, part), BF16),
            dma,
            dma((row_count + 1,)),
            dma((row_count + 1,)),
            dma((2,)),
            dma,
            dma((2,)),
            dma((lines, row_count)),
            dma((lines, row_count)),
            dma((lines + 1, row_count)),
        ],
        compiler_params=pltpu.CompilerParams(
            vmem_limit_bytes=63 * 1024 * 1024, has_side_effects=True
        ),
        cost_estimate=pl.CostEstimate(
            flops=8 * owned * lines * count * head_width,
            bytes_accessed=4 * count * head_width,
            transcendentals=heads * owned * col_count * count,
        ),
        name="attend",
    )(pixels, f, r, c, gain, rstd, rq, w_out)


def local(patches, w_patch, patch_bias, ln_gain, w_qkv, qk_gain, w_out):
    tile_rows, tile_cols, pix = patches.shape
    model_width = w_patch.shape[1]
    heads, size = w_qkv.shape[2], w_qkv.shape[3]
    head_width = heads * size
    col_count, row_count = lax.axis_size("col"), lax.axis_size("row")
    sizes = (row_count, col_count, tile_rows, tile_cols)
    grid_rows, grid_cols = tile_rows * row_count, tile_cols * col_count
    assert grid_cols % (tile_rows * tile_cols) == 0
    bias = patch_bias.astype(F32)[None, :]
    gain = ln_gain.astype(F32)[None, :]
    table = sincos_half(jnp.arange(max(grid_rows, grid_cols), dtype=jnp.int32), model_width)
    heads_w = w_qkv.transpose(1, 2, 0, 3).reshape(3 * heads, model_width, size)
    f, r, c, pixels, rstd = prep(
        patches.reshape(-1, pix), w_patch, gain, bias, table, heads_w, sizes, heads,
        grid_rows, grid_cols
    )
    rq = rstd[:, 0, :].reshape(row_count, col_count, tile_rows, tile_cols)
    rq = lax.dynamic_index_in_dim(rq, lax.axis_index("row"), 0, keepdims=False)
    rq = rq.transpose(1, 0, 2).reshape(col_count, tile_rows * tile_cols)
    exp_factor = math.log2(math.e) / math.sqrt(size)
    gains = jnp.concatenate(
        [qk_gain[0].reshape(1, -1) * exp_factor, qk_gain[1].reshape(1, -1)], axis=1
    )
    return attend(
        pixels, f, r, c, gains, rstd, rq, w_out.reshape(head_width, -1), sizes, heads, size
    )


def solution(mesh):
    return jax.shard_map(
        local,
        mesh=mesh,
        in_specs=(
            P("row", "col", None),
            P(),
            P(),
            P(),
            P(None, None, "col", None),
            P(None, "col", None),
            P("col", None, "row"),
        ),
        out_specs=P(("row", "col"), None),
        check_vma=False,
    )
```

```python
import functools
import math

import jax
import jax.numpy as jnp
from jax import lax
from jax.experimental import pallas as pl
from jax.experimental.pallas import tpu as pltpu
from jax.sharding import PartitionSpec as P

NORM_EPS = 1e-06
KEY_BLOCK = 1024
MISC = 16
F32 = jnp.float32
BF16 = jnp.bfloat16


def sincos_half(ids, model_width):
    quarter = model_width // 4
    frequency = 1.0 / 10000.0 ** (jnp.arange(quarter, dtype=jnp.float32) / quarter)
    angle = ids.astype(jnp.float32)[:, None] * frequency[None, :]
    return jnp.concatenate([jnp.sin(angle), jnp.cos(angle)], axis=1)


def ids():
    row, col = lax.axis_index("row"), lax.axis_index("col")
    return row, col, lax.div(col, 2), lax.rem(col, 2)


def row_peer(row, hop, count):
    if count != 4:
        return lax.rem(row + hop, count)
    if hop == 1:
        return row + 1 - 2 * lax.rem(row, 2)
    if hop == 2:
        return lax.rem(row + 2, 4)
    return 3 - row


def remote(src, dst, send, recv, row, col):
    return pltpu.make_async_remote_copy(
        src_ref=src, dst_ref=dst, send_sem=send, recv_sem=recv,
        device_id=(row, col), device_id_type=pl.DeviceIdType.MESH,
    )


def prep_kernel(sizes, group, centred_steps, patch_ref, wp_ref, gain_ref, bias_ref, table_ref,
                w_ref, wout_ref, f_ref, r_ref, c_ref, pixels_ref, rstd_ref, early_ref,
                a_ref, acc_ref, row_acc, e_ref, mean_ref, tmean_ref, mine_ref, seen_ref, held_ref,
                save_sem, send_sem, recv_sem, stat_send, stat_recv, early_send, early_recv):
    row_count, col_count, tile_rows, tile_cols = sizes
    step = pl.program_id(0)
    last = pl.num_programs(0) - 1
    pix, width = wp_ref.shape
    half = width // 2
    grid_rows, grid_cols = r_ref.shape[0], c_ref.shape[0]
    positions = table_ref.shape[0]
    base = pix + MISC
    tokens = tile_rows * tile_cols
    row, col, line, core = ids()
    me = row * col_count + col
    devices = row_count * col_count
    lines = col_count // 2
    partner = 2 * line + 1 - core

    relay = row_count == 4
    near = (1, 2) if relay else tuple(range(1, row_count))

    def early(side, portion):
        tall, piece = early_ref.shape[1] // 2, early_ref.shape[2]
        rows = pl.ds(portion * tall, tall)
        at = 2 * side + portion
        return remote(wout_ref.at[rows, pl.ds(side * piece, piece)], early_ref.at[side, rows],
                      early_send.at[at], early_recv.at[at],
                      row_peer(row, 1 + side, row_count), col)

    def give(src, block, to_row, to_col):
        remote(src, held_ref.at[block], send_sem, recv_sem.at[block], to_row, to_col).start()

    def save(block):
        pltpu.make_async_copy(held_ref.at[block], pixels_ref.at[block], save_sem).start()

    def got(block):
        pltpu.make_async_copy(held_ref.at[block], held_ref.at[block], recv_sem.at[block]).wait()
        save(block)

    def to_rows(src, block):
        for hop in near:
            give(src, block, row_peer(row, hop, row_count), col)

    @pl.when(step == 0)
    def _():
        for hop in range(1, lines):
            give(patch_ref, me, row, 2 * lax.rem(line + hop, lines) + core)
        to_rows(patch_ref, me)
        give(patch_ref, me, row, partner)
        pltpu.make_async_copy(patch_ref, pixels_ref.at[me], save_sem).start()
        if relay:
            for side in range(2):
                early(side, 0).start()
        gain = gain_ref[...]

        ones = jnp.ones((width, 128), BF16)
        tall = math.gcd(pix, 128)

        def average(i, carry):
            rows = pl.ds(pl.multiple_of(i * tall, tall), tall)
            total = jnp.dot(wp_ref[rows, :], ones, preferred_element_type=F32)
            mean_ref[rows, :] = total * (1.0 / width)
            return carry

        lax.fori_loop(0, pix // tall, average, 0)

        def centre(i, carry):
            rows = pl.ds(pl.multiple_of(i * 16, 16), 16)
            w = wp_ref[rows, :].astype(F32)
            a_ref[rows, :] = ((w - mean_ref[rows, 0:1]) * gain).astype(BF16)
            return carry

        lax.fori_loop(0, pix // 16, centre, 0)
        bias = bias_ref[...]
        bias = (bias - jnp.mean(bias, axis=1, keepdims=True)) * gain
        high = bias.astype(BF16).astype(F32)
        at = lax.broadcasted_iota(jnp.int32, (MISC, 1), 0)
        misc = jnp.where(at == 0, high, 0.0) + jnp.where(at == 1, bias - high, 0.0)
        a_ref[pix:base, :] = (misc + jnp.where(at == 2, gain, 0.0)).astype(BF16)

        def place(i, carry):
            rows = pl.ds(pl.multiple_of(i * 16, 16), 16)
            to = pl.ds(pl.multiple_of(base + i * 16, 16), 16)
            t = table_ref[rows, :]
            tmean_ref[rows, :] = jnp.broadcast_to(
                jnp.sum(t, axis=1, keepdims=True) * (1.0 / width), (16, 128)
            )
            a_ref[to, :half] = (t * gain[:, :half]).astype(BF16)
            a_ref[to, half:] = (t * gain[:, half:]).astype(BF16)
            return carry

        lax.fori_loop(0, positions // 16, place, 0)

    @pl.when(step == 1)
    def _():
        chunk = math.gcd(half, 512)
        own_rows = pl.ds(pl.multiple_of(row * tile_rows, 8), tile_rows)
        own_cols = pl.ds(pl.multiple_of(col * tile_cols, 8), tile_cols)
        shape = (tile_rows, tile_cols, chunk)

        def embed(i, carry):
            for side in range(2):
                at = pl.ds(pl.multiple_of(i * chunk, chunk), chunk)
                to = pl.ds(pl.multiple_of(side * half + i * chunk, chunk), chunk)
                if side == 0:
                    t = jnp.broadcast_to(table_ref[own_rows, at][:, None, :], shape)
                else:
                    t = jnp.broadcast_to(table_ref[own_cols, at][None, :, :], shape)
                e = jnp.dot(patch_ref[...], wp_ref[:, to], preferred_element_type=F32)
                e = e + bias_ref[:, to] + t.reshape(tokens, chunk)
                e_ref[:, to] = e
                for start in range(0, chunk, 128):
                    carry = carry + e[:, start : start + 128]
            return carry

        zero = jnp.zeros((tokens, 128), F32)
        total = lax.fori_loop(0, half // chunk, embed, zero)
        mean = jnp.sum(total, axis=1, keepdims=True) * (1.0 / width)

        def spread(i, carry):
            at = pl.ds(pl.multiple_of(i * chunk, chunk), chunk)
            e = e_ref[:, at] - mean
            for start in range(0, chunk, 128):
                part = e[:, start : start + 128]
                carry = carry + part * part
            return carry

        total = lax.fori_loop(0, width // chunk, spread, zero)
        variance = jnp.sum(total, axis=1, keepdims=True) * (1.0 / width)
        rstd = jnp.broadcast_to(lax.rsqrt(variance + NORM_EPS), (tokens, 128))
        mine_ref[...] = rstd.T[:8, :]

        def tell(hop, carry):
            to = lax.rem(me + hop, devices)
            remote(mine_ref, seen_ref.at[hop - 1], stat_send, stat_recv,
                   lax.div(to, col_count), lax.rem(to, col_count)).start()
            return carry

        lax.fori_loop(1, devices, tell, 0)
        seen_ref[devices - 1] = mine_ref[...]

    @pl.when(step == jnp.minimum(2, last))
    def _():
        for hop in range(1, lines):
            block = row * col_count + 2 * lax.rem(line + hop, lines) + core
            got(block)
            to_rows(held_ref.at[block], block)
            give(held_ref.at[block], block, row, partner)

    if relay:
        @pl.when(step == jnp.minimum(6, last))
        def _():
            for i in range(lines):
                for hop in (1, 2):
                    block = row_peer(row, hop, row_count) * col_count + 2 * i + core
                    got(block)
                    if (2 * i < lines) == (hop == 1):
                        give(held_ref.at[block], block, row_peer(row, 3 - hop, row_count), col)
                    give(held_ref.at[block], block, row, partner)
            for side in range(2):
                early(side, 1).start()

    def product(start):
        ks = slice(start, start + half)
        w = jnp.concatenate([w_ref[g, ks, :] for g in range(group)], axis=1)
        return jnp.dot(a_ref[:, ks], w, preferred_element_type=F32)

    acc_ref[...] = product(0)
    row_acc[...] = acc_ref[base : base + grid_rows, :]
    acc_ref[base:, :] = jnp.zeros((positions, acc_ref.shape[1]), F32)
    acc_ref[...] += product(half)
    bias_w = acc_ref[pix : pix + 1, :] + acc_ref[pix + 1 : pix + 2, :]
    gain_w = acc_ref[pix + 2 : pix + 3, :]
    r = row_acc[...] - tmean_ref[:grid_rows, 0:1] * gain_w
    c = acc_ref[base : base + grid_cols, :] - tmean_ref[:grid_cols, 0:1] * gain_w + bias_w
    f = acc_ref[:pix, :]
    size = f.shape[1] // group
    keep = jnp.where(step < centred_steps, 1.0, 0.0).astype(F32)
    for g in range(group):
        at = slice(g * size, (g + 1) * size)
        for value, out in ((f, f_ref), (r, r_ref), (c, c_ref)):
            part = value[:, at]
            part = part - keep * jnp.mean(part, axis=1, keepdims=True)
            out[:, at] = part.astype(out.dtype)

    @pl.when(step == last)
    def _():
        for hop in (3,) if relay else near:
            for i in range(lines):
                block = row_peer(row, hop, row_count) * col_count + 2 * i + core
                got(block)
                give(held_ref.at[block], block, row, partner)
        for other in range(row_count):
            for i in range(lines):
                got(other * col_count + 2 * i + 1 - core)
        everyone = held_ref.at[pl.ds(0, devices - 1)]
        pltpu.make_async_copy(everyone, everyone, send_sem).wait()
        seen = seen_ref.at[pl.ds(0, devices - 1)]
        pltpu.make_async_copy(seen, seen, stat_recv).wait()
        pltpu.make_async_copy(seen, seen, stat_send).wait()

        def put(block, carry):
            rstd_ref[block] = seen_ref[lax.rem(me - block + 2 * devices - 1, devices)]
            return carry

        lax.fori_loop(0, devices, put, 0)
        pltpu.make_async_copy(pixels_ref, pixels_ref, save_sem).wait()
        if relay:
            for side in range(2):
                early(side, 0).wait()
                early(side, 1).wait()


def prep(patches, w_patch, gain, bias, table, heads_w, w_out, sizes, heads_here, grid_rows, grid_cols):
    pix, width = w_patch.shape
    total, _, size = heads_w.shape
    group = next(g for g in (2, 3, 1) if heads_here % g == 0)
    steps = total // group
    positions = table.shape[0]
    rows = pix + MISC + positions
    tokens = patches.shape[0]
    devices = sizes[0] * sizes[1]
    whole = lambda s: pl.BlockSpec(s, lambda i: (0,) * len(s), pipeline_mode=pl.Buffered(1))
    return pl.pallas_call(
        functools.partial(prep_kernel, sizes, group, 2 * heads_here // group),
        grid=(steps,),
        in_specs=[
            whole((tokens, pix)),
            whole((pix, width)),
            whole((1, width)),
            whole((1, width)),
            whole(table.shape),
            pl.BlockSpec((group, width, size), lambda i: (i, 0, 0)),
            pl.BlockSpec(memory_space=pl.ANY),
        ],
        out_specs=[
            pl.BlockSpec((pix, group * size), lambda i: (0, i)),
            pl.BlockSpec((grid_rows, group * size), lambda i: (0, i)),
            pl.BlockSpec((grid_cols, group * size), lambda i: (0, i)),
            pl.BlockSpec(memory_space=pl.ANY),
            pl.BlockSpec((devices, 8, tokens), lambda i: (0, 0, 0)),
            pl.BlockSpec(memory_space=pl.ANY),
        ],
        out_shape=[
            jax.ShapeDtypeStruct((pix, total * size), BF16),
            jax.ShapeDtypeStruct((grid_rows, total * size), F32),
            jax.ShapeDtypeStruct((grid_cols, total * size), F32),
            jax.ShapeDtypeStruct((devices, tokens, pix), BF16),
            jax.ShapeDtypeStruct((devices, 8, tokens), F32),
            jax.ShapeDtypeStruct((2, w_out.shape[0], w_out.shape[1] // 2), BF16),
        ],
        scratch_shapes=[
            pltpu.VMEM((rows, width), BF16),
            pltpu.VMEM((rows, group * size), F32),
            pltpu.VMEM((grid_rows, group * size), F32),
            pltpu.VMEM((tokens, width), F32),
            pltpu.VMEM((pix, 128), F32),
            pltpu.VMEM((positions, 128), F32),
            pltpu.VMEM((8, tokens), F32),
            pltpu.VMEM((devices, 8, tokens), F32),
            pltpu.VMEM((devices, tokens, pix), BF16),
            pltpu.SemaphoreType.DMA,
            pltpu.SemaphoreType.DMA,
            pltpu.SemaphoreType.DMA((devices,)),
            pltpu.SemaphoreType.DMA,
            pltpu.SemaphoreType.DMA,
            pltpu.SemaphoreType.DMA((4,)),
            pltpu.SemaphoreType.DMA((4,)),
        ],
        compiler_params=pltpu.CompilerParams(
            dimension_semantics=("arbitrary",), vmem_limit_bytes=60 * 1024 * 1024,
            has_side_effects=True,
        ),
        cost_estimate=pl.CostEstimate(
            flops=2 * rows * width * total * size,
            bytes_accessed=2 * width * total * size,
            transcendentals=0,
        ),
        name="prep",
    )(patches, w_patch, gain, bias, table, heads_w, w_out)

def attention_block(key_block, query, k_ref, v_ref):
    rows, head_size = query.shape
    peak = jnp.full((rows, 1), -1e30, F32)
    total = jnp.zeros((rows, 1), F32)
    acc = jnp.zeros((rows, head_size), F32)
    for start in range(0, k_ref.shape[0], key_block):
        scores = lax.dot_general(
            query,
            k_ref[start : start + key_block, :],
            (((1,), (1,)), ((), ())),
            preferred_element_type=F32,
        )
        new_peak = jnp.maximum(peak, jnp.max(scores, axis=1, keepdims=True))
        rescale = jnp.exp2(peak - new_peak)
        weights = jnp.exp2(scores - new_peak)
        total = total * rescale + jnp.sum(weights, axis=1, keepdims=True)
        acc = acc * rescale + jnp.dot(
            weights.astype(BF16), v_ref[start : start + key_block, :], preferred_element_type=F32
        )
        peak = new_peak
    return (acc / total).astype(BF16)


def attend_kernel(sizes, heads, key_block, pixels_ref, f_ref, r_ref, c_ref, gain_ref, rstd_ref,
                  rq_ref, w_ref, early_ref, out_ref, kv_ref, wall_ref, pbuf_ref, qbuf_ref, q_ref, ctx_ref,
                  pair_ref, hop_ref, own_ref, stage_ref, w_local, early_sem, w_send, w_recv, p_sem, q_sem,
                  stage_send, pair_recv, hop_send, hop_recv):
    row_count, col_count, tile_rows, tile_cols = sizes
    row, col, line, core = ids()
    lines = col_count // 2
    partner = 2 * line + 1 - core
    size = kv_ref.shape[2]
    head_width = heads * size
    blocks, tokens, pix = pbuf_ref.shape[1:]
    owned = tile_cols * tile_rows
    per_line = tile_cols * col_count // owned
    part = wall_ref.shape[2]
    wide = 2 * size
    exp_factor = math.log2(math.e) / math.sqrt(size)
    is_end = jnp.logical_or(line == 0, line == lines - 1)

    def wait(ref, sem):
        pltpu.make_async_copy(ref, ref, sem).wait()

    def order(s):
        up = jnp.where(s < lines - 1 - line, lines - 1 - s, s - (lines - 1 - line))
        down = jnp.where(s < line, s, lines - 1 - (s - line))
        far = jnp.where(2 * line < lines, up, down)
        return jnp.where(s == lines - 1, line, far)

    relay = row_count == 4
    piece = part // 2

    def half(side):
        return pl.ds(side * piece, piece)

    def load_early(side):
        return pltpu.make_async_copy(
            early_ref.at[side], wall_ref.at[1 + side, :, half(side)], early_sem.at[side]
        )

    def rest(side):
        at = half(1 - side)
        return remote(wall_ref.at[0, :, at], wall_ref.at[1 + side, :, at], w_send.at[1 + side],
                      w_recv.at[1 + side], row_peer(row, 1 + side, row_count), col)

    def relayed(side):
        at = half(side)
        return remote(wall_ref.at[1 + side, :, at], wall_ref.at[3, :, at], w_send.at[3 + side],
                      w_recv.at[3 + side], row_peer(row, 2 - side, row_count), col)

    fetch_w = pltpu.make_async_copy(w_ref, wall_ref.at[0], w_local)
    fetch_w.start()
    if relay:
        load_early(0).start()
        load_early(1).start()

    def fetch(i):
        slot = lax.rem(i, 2)
        return pltpu.make_async_copy(
            pixels_ref.at[pl.ds(i * blocks, blocks)], pbuf_ref.at[slot], p_sem.at[slot]
        )

    def q_row(s, side):
        return 2 * order(s) + (core if side else 1 - core)

    def fetch_q(s):
        for side in range(2):
            mine = q_row(s, side)
            first = lax.rem(mine, per_line) * tile_rows
            lane = pl.multiple_of(lax.div(mine, per_line) * tile_cols, tile_cols)
            for c in range(tile_rows):
                pltpu.make_async_copy(
                    pixels_ref.at[row * col_count + first + c, pl.ds(lane, tile_cols), :],
                    qbuf_ref.at[pl.ds(side * owned + c * tile_cols, tile_cols), :],
                    q_sem,
                ).start()

    def pick(rows, index):
        at = lax.broadcasted_iota(jnp.int32, rows.shape, 0)
        return jnp.sum(jnp.where(at == index, rows, 0.0), axis=0, keepdims=True)

    def normed(x, scale_rows, gain):
        square = jnp.sum(x * x, axis=1, keepdims=True) * (1.0 / size)
        return x * (scale_rows * lax.rsqrt(square * scale_rows * scale_rows + NORM_EPS)) * gain

    fetch(0).start()
    fetch_q(0)
    fetch_w.wait()
    if relay:
        for side in range(2):
            rest(side).start()
        for side in range(2):
            load_early(side).wait()
            relayed(side).start()
    else:
        for hop in range(1, row_count):
            remote(wall_ref.at[0], wall_ref.at[hop], w_send.at[hop], w_recv.at[hop],
                   row_peer(row, hop, row_count), col).start()
    rounds = pixels_ref.shape[0] // blocks

    def keys_values(i, carry):
        fetch(i).wait()

        @pl.when(i + 1 < rounds)
        def _():
            fetch(i + 1).start()

        p = pbuf_ref[lax.rem(i, 2)].reshape(blocks * tokens, pix)
        rstd = []
        for b in range(blocks):
            lanes = rstd_ref[i * blocks + b][0:1, :]
            rstd.append(jnp.broadcast_to(lanes, (size, tokens)).T)
        for start in range(0, 2 * head_width, wide):
            at = slice(head_width + start, head_width + start + wide)
            x = jnp.dot(p, f_ref[:, at], preferred_element_type=F32)
            for b in range(blocks):
                block = i * blocks + b
                rows = pl.ds(pl.multiple_of(lax.div(block, col_count) * tile_rows, 8), tile_rows)
                cols = pl.ds(pl.multiple_of(lax.rem(block, col_count) * tile_cols, 8), tile_cols)
                u = c_ref[cols, at][None, :, :] + r_ref[rows, at][:, None, :]
                y = x[b * tokens : (b + 1) * tokens] + u.reshape(tokens, wide)
                to = pl.ds(pl.multiple_of(block * tokens, tokens), tokens)
                for g in range(2):
                    head = start // size + g
                    z = y[:, g * size : (g + 1) * size]
                    if head < heads:
                        gain = gain_ref[1:2, head * size : (head + 1) * size]
                        z = normed(z, rstd[b], gain)
                    else:
                        z = z * rstd[b]
                    kv_ref[head, to, :] = z.astype(BF16)
        return carry

    lax.fori_loop(0, rounds, keys_values, 0)

    def attend(s):
        wait(qbuf_ref, q_sem)
        own_rows = pl.ds(pl.multiple_of(row * tile_rows, 8), tile_rows)
        sides = []
        for side in range(2):
            mine = q_row(s, side)
            cols = pl.ds(pl.multiple_of(lax.rem(mine, per_line) * owned, owned), owned)
            rstd = jnp.broadcast_to(pick(rq_ref[...], mine), (size, owned)).T
            sides.append((lax.div(mine, per_line), cols, rstd))
        step_width = wide if head_width % wide == 0 else size
        for start in range(0, head_width, step_width):
            span = slice(start, start + step_width)
            x = jnp.dot(qbuf_ref[...], f_ref[:, span], preferred_element_type=F32)
            for g in range(step_width // size):
                at = slice(start + g * size, start + (g + 1) * size)
                for side, (line_row, cols, rstd) in enumerate(sides):
                    rows = slice(side * owned, (side + 1) * owned)
                    y = x[rows, g * size : (g + 1) * size]
                    y = y + (c_ref[cols, at] + pick(r_ref[own_rows, at], line_row))
                    y = normed(y, rstd, gain_ref[0:1, at] * exp_factor)
                    q_ref[start // size + g, rows, :] = y.astype(BF16)

        @pl.when(s + 1 < lines)
        def _():
            fetch_q(s + 1)

        def one_head(h, carry):
            to = pl.ds(pl.multiple_of(h * size, size), size)
            ctx_ref[s, :, to] = attention_block(
                key_block, q_ref[h], kv_ref.at[h], kv_ref.at[heads + h]
            )
            return carry

        lax.fori_loop(0, heads, one_head, 0)

    chunk = math.gcd(part, 512)

    def project_out(n, s, j):
        slot = lax.rem(n, 2)
        dest = order(s)

        @pl.when(n >= 2)
        def _():
            wait(stage_ref.at[slot], stage_send.at[slot])

        def columns(i, carry):
            at = pl.ds(pl.multiple_of(i * chunk, chunk), chunk)
            x = jnp.dot(ctx_ref[s], wall_ref[j, :, at], preferred_element_type=F32).astype(BF16)
            stage_ref[slot, :, at] = x[:owned]
            own_ref[slot, :, at] = x[owned:]
            return carry

        lax.fori_loop(0, part // chunk, columns, 0)
        remote(stage_ref.at[slot], pair_ref.at[dest, j], stage_send.at[slot],
               pair_recv.at[dest, j], row, partner).start()

    def settle(n, s, j):
        dest = order(s)
        own = own_ref[lax.rem(n, 2)].astype(F32)
        wait(pair_ref.at[dest, j], pair_recv.at[dest, j])
        pair_ref[dest, j] = (pair_ref[dest, j].astype(F32) + own).astype(BF16)

        @pl.when(jnp.logical_and(is_end, s < lines - 1))
        def _():
            pass_on(s, j)

    def pass_on(s, j):
        dest = order(s)
        up = dest > line
        to = jnp.where(up, line + 1, line - 1)
        slot = jnp.where(jnp.logical_and(dest == to, jnp.logical_not(up)), lines, dest)

        @pl.when(jnp.logical_not(is_end))
        def _():
            wait(hop_ref.at[dest, j], hop_recv.at[dest, j])
            total = pair_ref[dest, j].astype(F32) + hop_ref[dest, j].astype(F32)
            pair_ref[dest, j] = total.astype(BF16)

        remote(pair_ref.at[dest, j], hop_ref.at[slot, j], hop_send.at[dest, j],
               hop_recv.at[slot, j], row, 2 * to + core).start()

    inner = row_count - 1

    def group_start(s):
        return s * inner

    def step(s, carry):
        attend(s)

        @pl.when(s == 0)
        def _():
            if relay:
                for side in range(2):
                    rest(side).wait_recv()
            else:
                for hop in range(1, row_count - 1):
                    wait(wall_ref.at[hop], w_recv.at[hop])

        def make(t, c):
            project_out(group_start(s) + t, s, t)

            @pl.when(t > 0)
            def _():
                settle(group_start(s) + t - 1, s, t - 1)

            return c

        lax.fori_loop(0, inner, make, 0)
        settle(group_start(s) + inner - 1, s, inner - 1)

        @pl.when(jnp.logical_and(s > 0, jnp.logical_not(is_end)))
        def _():
            def late(t, c):
                pass_on(s - 1, t)
                return c

            lax.fori_loop(0, inner, late, 0)

        return carry

    lax.fori_loop(0, lines, step, 0)
    final = row_count - 1
    if relay:
        for side in range(2):
            relayed(side).wait_recv()
    else:
        wait(wall_ref.at[final], w_recv.at[final])

    def make_last(s, c):
        project_out(group_start(lines) + s, s, final)

        @pl.when(s > 0)
        def _():
            settle(group_start(lines) + s - 1, s - 1, final)

        return c

    lax.fori_loop(0, lines, make_last, 0)
    settle(group_start(lines) + lines - 1, lines - 1, final)

    def finish(j, sender):
        to = pl.ds(pl.multiple_of(sender * part, 128), part)
        side = jnp.where(line > 0, line, lines)
        wait(hop_ref.at[side, j], hop_recv.at[side, j])

        @pl.when(is_end)
        def _():
            total = pair_ref[line, j].astype(F32) + hop_ref[side, j].astype(F32)
            out_ref[:, to] = total.astype(BF16)

        @pl.when(jnp.logical_not(is_end))
        def _():
            wait(hop_ref.at[lines, j], hop_recv.at[lines, j])
            total = pair_ref[line, j].astype(F32) + hop_ref[line, j].astype(F32)
            out_ref[:, to] = (total + hop_ref[lines, j].astype(F32)).astype(BF16)

    def sender_of(hop):
        if hop == 0:
            return row
        if row_count == 4:
            return row_peer(row, hop, row_count)
        return lax.rem(row + row_count - hop, row_count)

    for j in range(row_count - 1):
        finish(j, sender_of(j))

    @pl.when(jnp.logical_not(is_end))
    def _():
        def late(s, c):
            pass_on(s, final)
            return c

        lax.fori_loop(0, lines - 1, late, 0)

    finish(final, sender_of(final))
    if relay:
        for side in range(2):
            rest(side).wait_send()
            relayed(side).wait_send()
    else:
        for hop in range(1, row_count):
            wait(wall_ref.at[0], w_send.at[hop])
    for slot in range(2):
        wait(stage_ref.at[slot], stage_send.at[slot])

    def drain(s, c):
        for j in range(row_count):
            wait(pair_ref.at[order(s), j], hop_send.at[order(s), j])
        return c

    lax.fori_loop(0, lines - 1, drain, 0)


def attend(pixels, f, r, c, gain, rstd, rq, w_out, early, sizes, heads, size):
    row_count, col_count, tile_rows, tile_cols = sizes
    devices, tokens, pix = pixels.shape
    head_width, part = w_out.shape
    lines = col_count // 2
    owned = tile_cols * tile_rows
    count = devices * tokens
    blocks = math.gcd(devices, 4)
    vmem = lambda: pl.BlockSpec(memory_space=pltpu.VMEM)
    hbm = lambda: pl.BlockSpec(memory_space=pl.ANY)
    dma = pltpu.SemaphoreType.DMA
    return pl.pallas_call(
        functools.partial(attend_kernel, sizes, heads, math.gcd(count, KEY_BLOCK)),
        in_specs=[hbm(), vmem(), vmem(), vmem(), vmem(), vmem(), vmem(), hbm(), hbm()],
        out_specs=vmem(),
        out_shape=jax.ShapeDtypeStruct((owned, part * row_count), BF16),
        scratch_shapes=[
            pltpu.VMEM((2 * heads, count, size), BF16),
            pltpu.VMEM((row_count, head_width, part), BF16),
            pltpu.VMEM((2, blocks, tokens, pix), BF16),
            pltpu.VMEM((2 * owned, pix), BF16),
            pltpu.VMEM((heads, 2 * owned, size), BF16),
            pltpu.VMEM((lines, 2 * owned, head_width), BF16),
            pltpu.VMEM((lines, row_count, owned, part), BF16),
            pltpu.VMEM((lines + 1, row_count, owned, part), BF16),
            pltpu.VMEM((2, owned, part), BF16),
            pltpu.VMEM((2, owned, part), BF16),
            dma,
            dma((2,)),
            dma((row_count + 1,)),
            dma((row_count + 1,)),
            dma((2,)),
            dma,
            dma((2,)),
            dma((lines, row_count)),
            dma((lines, row_count)),
            dma((lines + 1, row_count)),
        ],
        compiler_params=pltpu.CompilerParams(
            vmem_limit_bytes=63 * 1024 * 1024, has_side_effects=True
        ),
        cost_estimate=pl.CostEstimate(
            flops=8 * owned * lines * count * head_width,
            bytes_accessed=4 * count * head_width,
            transcendentals=heads * owned * col_count * count,
        ),
        name="attend",
    )(pixels, f, r, c, gain, rstd, rq, w_out, early)


def local(patches, w_patch, patch_bias, ln_gain, w_qkv, qk_gain, w_out):
    tile_rows, tile_cols, pix = patches.shape
    model_width = w_patch.shape[1]
    heads, size = w_qkv.shape[2], w_qkv.shape[3]
    head_width = heads * size
    col_count, row_count = lax.axis_size("col"), lax.axis_size("row")
    sizes = (row_count, col_count, tile_rows, tile_cols)
    grid_rows, grid_cols = tile_rows * row_count, tile_cols * col_count
    assert grid_cols % (tile_rows * tile_cols) == 0
    bias = patch_bias.astype(F32)[None, :]
    gain = ln_gain.astype(F32)[None, :]
    table = sincos_half(jnp.arange(max(grid_rows, grid_cols), dtype=jnp.int32), model_width)
    heads_w = w_qkv.transpose(1, 2, 0, 3).reshape(3 * heads, model_width, size)
    out_rows = w_out.reshape(head_width, -1)
    f, r, c, pixels, rstd, early = prep(
        patches.reshape(-1, pix), w_patch, gain, bias, table, heads_w, out_rows, sizes, heads,
        grid_rows, grid_cols
    )
    rq = rstd[:, 0, :].reshape(row_count, col_count, tile_rows, tile_cols)
    rq = lax.dynamic_index_in_dim(rq, lax.axis_index("row"), 0, keepdims=False)
    rq = rq.transpose(1, 0, 2).reshape(col_count, tile_rows * tile_cols)
    gains = qk_gain.reshape(2, head_width)
    return attend(
        pixels, f, r, c, gains, rstd, rq, out_rows, early, sizes, heads, size
    )


def solution(mesh):
    return jax.shard_map(
        local,
        mesh=mesh,
        in_specs=(
            P("row", "col", None),
            P(),
            P(),
            P(),
            P(None, None, "col", None),
            P(None, "col", None),
            P("col", None, "row"),
        ),
        out_specs=P(("row", "col"), None),
        check_vma=False,
    )
```

```python
import functools
import math

import jax
import jax.numpy as jnp
from jax import lax
from jax.experimental import pallas as pl
from jax.experimental.pallas import tpu as pltpu
from jax.sharding import PartitionSpec as P

NORM_EPS = 1e-06
KEY_BLOCK = 1024
MISC = 16
F32 = jnp.float32
BF16 = jnp.bfloat16


def sincos_half(ids, model_width):
    quarter = model_width // 4
    frequency = 1.0 / 10000.0 ** (jnp.arange(quarter, dtype=jnp.float32) / quarter)
    angle = ids.astype(jnp.float32)[:, None] * frequency[None, :]
    return jnp.concatenate([jnp.sin(angle), jnp.cos(angle)], axis=1)


def ids():
    row, col = lax.axis_index("row"), lax.axis_index("col")
    return row, col, lax.div(col, 2), lax.rem(col, 2)


def row_peer(row, hop, count):
    if count != 4:
        return lax.rem(row + hop, count)
    if hop == 1:
        return row + 1 - 2 * lax.rem(row, 2)
    if hop == 2:
        return lax.rem(row + 2, 4)
    return 3 - row


def remote(src, dst, send, recv, row, col):
    return pltpu.make_async_remote_copy(
        src_ref=src, dst_ref=dst, send_sem=send, recv_sem=recv,
        device_id=(row, col), device_id_type=pl.DeviceIdType.MESH,
    )


def prep_kernel(sizes, group, centred_steps, patch_ref, wp_ref, gain_ref, bias_ref, table_ref,
                w_ref, wout_ref, f_ref, r_ref, c_ref, pixels_ref, rstd_ref, early_ref,
                a_ref, acc_ref, row_acc, e_ref, mean_ref, tmean_ref, mine_ref, seen_ref, held_ref,
                save_sem, send_sem, recv_sem, stat_send, stat_recv, early_send, early_recv):
    row_count, col_count, tile_rows, tile_cols = sizes
    step = pl.program_id(0)
    last = pl.num_programs(0) - 1
    pix, width = wp_ref.shape
    half = width // 2
    grid_rows, grid_cols = r_ref.shape[0], c_ref.shape[0]
    positions = table_ref.shape[0]
    base = pix + MISC
    tokens = tile_rows * tile_cols
    row, col, line, core = ids()
    me = row * col_count + col
    devices = row_count * col_count
    lines = col_count // 2
    partner = 2 * line + 1 - core

    relay = row_count == 4
    near = (1, 2) if relay else tuple(range(1, row_count))

    def early(side, portion):
        tall, piece = early_ref.shape[1] // 2, early_ref.shape[2]
        rows = pl.ds(portion * tall, tall)
        at = 2 * side + portion
        return remote(wout_ref.at[rows, pl.ds(side * piece, piece)], early_ref.at[side, rows],
                      early_send.at[at], early_recv.at[at],
                      row_peer(row, 1 + side, row_count), col)

    def give(src, block, to_row, to_col):
        remote(src, held_ref.at[block], send_sem, recv_sem.at[block], to_row, to_col).start()

    def save(block):
        pltpu.make_async_copy(held_ref.at[block], pixels_ref.at[block], save_sem).start()

    def got(block):
        pltpu.make_async_copy(held_ref.at[block], held_ref.at[block], recv_sem.at[block]).wait()
        save(block)

    def to_rows(src, block):
        for hop in near:
            give(src, block, row_peer(row, hop, row_count), col)

    @pl.when(step == 0)
    def _():
        for hop in range(1, lines):
            give(patch_ref, me, row, 2 * lax.rem(line + hop, lines) + core)
        to_rows(patch_ref, me)
        give(patch_ref, me, row, partner)
        pltpu.make_async_copy(patch_ref, pixels_ref.at[me], save_sem).start()
        if relay:
            for side in range(2):
                early(side, 0).start()
        gain = gain_ref[...]

        ones = jnp.ones((width, 128), BF16)
        tall = math.gcd(pix, 128)

        def average(i, carry):
            rows = pl.ds(pl.multiple_of(i * tall, tall), tall)
            total = jnp.dot(wp_ref[rows, :], ones, preferred_element_type=F32)
            mean_ref[rows, :] = total * (1.0 / width)
            return carry

        lax.fori_loop(0, pix // tall, average, 0)

        def centre(i, carry):
            rows = pl.ds(pl.multiple_of(i * 16, 16), 16)
            w = wp_ref[rows, :].astype(F32)
            a_ref[rows, :] = ((w - mean_ref[rows, 0:1]) * gain).astype(BF16)
            return carry

        lax.fori_loop(0, pix // 16, centre, 0)
        bias = bias_ref[...]
        bias = (bias - jnp.mean(bias, axis=1, keepdims=True)) * gain
        high = bias.astype(BF16).astype(F32)
        at = lax.broadcasted_iota(jnp.int32, (MISC, 1), 0)
        misc = jnp.where(at == 0, high, 0.0) + jnp.where(at == 1, bias - high, 0.0)
        a_ref[pix:base, :] = (misc + jnp.where(at == 2, gain, 0.0)).astype(BF16)

        def place(i, carry):
            rows = pl.ds(pl.multiple_of(i * 16, 16), 16)
            to = pl.ds(pl.multiple_of(base + i * 16, 16), 16)
            t = table_ref[rows, :]
            tmean_ref[rows, :] = jnp.broadcast_to(
                jnp.sum(t, axis=1, keepdims=True) * (1.0 / width), (16, 128)
            )
            a_ref[to, :half] = (t * gain[:, :half]).astype(BF16)
            a_ref[to, half:] = (t * gain[:, half:]).astype(BF16)
            return carry

        lax.fori_loop(0, positions // 16, place, 0)

    @pl.when(step == jnp.minimum(3, last))
    def _():
        chunk = math.gcd(half, 512)
        own_rows = pl.ds(pl.multiple_of(row * tile_rows, 8), tile_rows)
        own_cols = pl.ds(pl.multiple_of(col * tile_cols, 8), tile_cols)
        shape = (tile_rows, tile_cols, chunk)

        def embed(i, carry):
            for side in range(2):
                at = pl.ds(pl.multiple_of(i * chunk, chunk), chunk)
                to = pl.ds(pl.multiple_of(side * half + i * chunk, chunk), chunk)
                if side == 0:
                    t = jnp.broadcast_to(table_ref[own_rows, at][:, None, :], shape)
                else:
                    t = jnp.broadcast_to(table_ref[own_cols, at][None, :, :], shape)
                e = jnp.dot(patch_ref[...], wp_ref[:, to], preferred_element_type=F32)
                e = e + bias_ref[:, to] + t.reshape(tokens, chunk)
                e_ref[:, to] = e
                for start in range(0, chunk, 128):
                    carry = carry + e[:, start : start + 128]
            return carry

        zero = jnp.zeros((tokens, 128), F32)
        total = lax.fori_loop(0, half // chunk, embed, zero)
        mean = jnp.sum(total, axis=1, keepdims=True) * (1.0 / width)

        def spread(i, carry):
            at = pl.ds(pl.multiple_of(i * chunk, chunk), chunk)
            e = e_ref[:, at] - mean
            for start in range(0, chunk, 128):
                part = e[:, start : start + 128]
                carry = carry + part * part
            return carry

        total = lax.fori_loop(0, width // chunk, spread, zero)
        variance = jnp.sum(total, axis=1, keepdims=True) * (1.0 / width)
        rstd = jnp.broadcast_to(lax.rsqrt(variance + NORM_EPS), (tokens, 128))
        mine_ref[...] = rstd.T[:8, :]

        def tell(hop, carry):
            to = lax.rem(me + hop, devices)
            remote(mine_ref, seen_ref.at[hop - 1], stat_send, stat_recv,
                   lax.div(to, col_count), lax.rem(to, col_count)).start()
            return carry

        lax.fori_loop(1, devices, tell, 0)
        seen_ref[devices - 1] = mine_ref[...]

    @pl.when(step == jnp.minimum(2, last))
    def _():
        for hop in range(1, lines):
            block = row * col_count + 2 * lax.rem(line + hop, lines) + core
            got(block)
            to_rows(held_ref.at[block], block)
            give(held_ref.at[block], block, row, partner)

    if relay:
        @pl.when(step == jnp.minimum(5, last))
        def _():
            for i in range(lines):
                for hop in (1, 2):
                    block = row_peer(row, hop, row_count) * col_count + 2 * i + core
                    got(block)
                    if (2 * i < lines) == (hop == 1):
                        give(held_ref.at[block], block, row_peer(row, 3 - hop, row_count), col)
                    give(held_ref.at[block], block, row, partner)
            for side in range(2):
                early(side, 1).start()

    def product(start):
        ks = slice(start, start + half)
        w = jnp.concatenate([w_ref[g, ks, :] for g in range(group)], axis=1)
        return jnp.dot(a_ref[:, ks], w, preferred_element_type=F32)

    acc_ref[...] = product(0)
    row_acc[...] = acc_ref[base : base + grid_rows, :]
    acc_ref[base:, :] = jnp.zeros((positions, acc_ref.shape[1]), F32)
    acc_ref[...] += product(half)
    bias_w = acc_ref[pix : pix + 1, :] + acc_ref[pix + 1 : pix + 2, :]
    gain_w = acc_ref[pix + 2 : pix + 3, :]
    r = row_acc[...] - tmean_ref[:grid_rows, 0:1] * gain_w
    c = acc_ref[base : base + grid_cols, :] - tmean_ref[:grid_cols, 0:1] * gain_w + bias_w
    f = acc_ref[:pix, :]
    size = f.shape[1] // group
    keep = jnp.where(step < centred_steps, 1.0, 0.0).astype(F32)
    for g in range(group):
        at = slice(g * size, (g + 1) * size)
        for value, out in ((f, f_ref), (r, r_ref), (c, c_ref)):
            part = value[:, at]
            part = part - keep * jnp.mean(part, axis=1, keepdims=True)
            out[:, at] = part.astype(out.dtype)

    @pl.when(step == last)
    def _():
        for hop in (3,) if relay else near:
            for i in range(lines):
                block = row_peer(row, hop, row_count) * col_count + 2 * i + core
                got(block)
                give(held_ref.at[block], block, row, partner)
        for other in range(row_count):
            for i in range(lines):
                got(other * col_count + 2 * i + 1 - core)
        everyone = held_ref.at[pl.ds(0, devices - 1)]
        pltpu.make_async_copy(everyone, everyone, send_sem).wait()
        seen = seen_ref.at[pl.ds(0, devices - 1)]
        pltpu.make_async_copy(seen, seen, stat_recv).wait()
        pltpu.make_async_copy(seen, seen, stat_send).wait()

        def put(block, carry):
            rstd_ref[block] = seen_ref[lax.rem(me - block + 2 * devices - 1, devices)]
            return carry

        lax.fori_loop(0, devices, put, 0)
        pltpu.make_async_copy(pixels_ref, pixels_ref, save_sem).wait()
        if relay:
            for side in range(2):
                early(side, 0).wait()
                early(side, 1).wait()


def prep(patches, w_patch, gain, bias, table, heads_w, w_out, sizes, heads_here, grid_rows, grid_cols):
    pix, width = w_patch.shape
    total, _, size = heads_w.shape
    group = next(g for g in (2, 3, 1) if heads_here % g == 0)
    steps = total // group
    positions = table.shape[0]
    rows = pix + MISC + positions
    tokens = patches.shape[0]
    devices = sizes[0] * sizes[1]
    whole = lambda s: pl.BlockSpec(s, lambda i: (0,) * len(s), pipeline_mode=pl.Buffered(1))
    return pl.pallas_call(
        functools.partial(prep_kernel, sizes, group, 2 * heads_here // group),
        grid=(steps,),
        in_specs=[
            whole((tokens, pix)),
            whole((pix, width)),
            whole((1, width)),
            whole((1, width)),
            whole(table.shape),
            pl.BlockSpec((group, width, size), lambda i: (i, 0, 0)),
            pl.BlockSpec(memory_space=pl.ANY),
        ],
        out_specs=[
            pl.BlockSpec((pix, group * size), lambda i: (0, i)),
            pl.BlockSpec((grid_rows, group * size), lambda i: (0, i)),
            pl.BlockSpec((grid_cols, group * size), lambda i: (0, i)),
            pl.BlockSpec(memory_space=pl.ANY),
            pl.BlockSpec((devices, 8, tokens), lambda i: (0, 0, 0)),
            pl.BlockSpec(memory_space=pl.ANY),
        ],
        out_shape=[
            jax.ShapeDtypeStruct((pix, total * size), BF16),
            jax.ShapeDtypeStruct((grid_rows, total * size), F32),
            jax.ShapeDtypeStruct((grid_cols, total * size), F32),
            jax.ShapeDtypeStruct((devices, tokens, pix), BF16),
            jax.ShapeDtypeStruct((devices, 8, tokens), F32),
            jax.ShapeDtypeStruct((2, w_out.shape[0], w_out.shape[1] // 2), BF16),
        ],
        scratch_shapes=[
            pltpu.VMEM((rows, width), BF16),
            pltpu.VMEM((rows, group * size), F32),
            pltpu.VMEM((grid_rows, group * size), F32),
            pltpu.VMEM((tokens, width), F32),
            pltpu.VMEM((pix, 128), F32),
            pltpu.VMEM((positions, 128), F32),
            pltpu.VMEM((8, tokens), F32),
            pltpu.VMEM((devices, 8, tokens), F32),
            pltpu.VMEM((devices, tokens, pix), BF16),
            pltpu.SemaphoreType.DMA,
            pltpu.SemaphoreType.DMA,
            pltpu.SemaphoreType.DMA((devices,)),
            pltpu.SemaphoreType.DMA,
            pltpu.SemaphoreType.DMA,
            pltpu.SemaphoreType.DMA((4,)),
            pltpu.SemaphoreType.DMA((4,)),
        ],
        compiler_params=pltpu.CompilerParams(
            dimension_semantics=("arbitrary",), vmem_limit_bytes=60 * 1024 * 1024,
            has_side_effects=True,
        ),
        cost_estimate=pl.CostEstimate(
            flops=2 * rows * width * total * size,
            bytes_accessed=2 * width * total * size,
            transcendentals=0,
        ),
        name="prep",
    )(patches, w_patch, gain, bias, table, heads_w, w_out)

def attention_block(key_block, query, k_ref, v_ref):
    rows, head_size = query.shape
    peak = jnp.full((rows, 1), -1e30, F32)
    total = jnp.zeros((rows, 1), F32)
    acc = jnp.zeros((rows, head_size), F32)
    for start in range(0, k_ref.shape[0], key_block):
        scores = lax.dot_general(
            query,
            k_ref[start : start + key_block, :],
            (((1,), (1,)), ((), ())),
            preferred_element_type=F32,
        )
        new_peak = jnp.maximum(peak, jnp.max(scores, axis=1, keepdims=True))
        rescale = jnp.exp2(peak - new_peak)
        weights = jnp.exp2(scores - new_peak)
        total = total * rescale + jnp.sum(weights, axis=1, keepdims=True)
        acc = acc * rescale + jnp.dot(
            weights.astype(BF16), v_ref[start : start + key_block, :], preferred_element_type=F32
        )
        peak = new_peak
    return (acc / total).astype(BF16)


def attend_kernel(sizes, heads, key_block, pixels_ref, f_ref, r_ref, c_ref, gain_ref, rstd_ref,
                  rq_ref, w_ref, early_ref, out_ref, kv_ref, wall_ref, pbuf_ref, qbuf_ref, q_ref, ctx_ref,
                  pair_ref, hop_ref, own_ref, stage_ref, w_local, early_sem, w_send, w_recv, p_sem, q_sem,
                  stage_send, pair_recv, hop_send, hop_recv):
    row_count, col_count, tile_rows, tile_cols = sizes
    row, col, line, core = ids()
    lines = col_count // 2
    partner = 2 * line + 1 - core
    size = kv_ref.shape[2]
    head_width = heads * size
    blocks, tokens, pix = pbuf_ref.shape[1:]
    owned = tile_cols * tile_rows
    per_line = tile_cols * col_count // owned
    part = wall_ref.shape[2]
    wide = 2 * size
    exp_factor = math.log2(math.e) / math.sqrt(size)
    is_end = jnp.logical_or(line == 0, line == lines - 1)

    def wait(ref, sem):
        pltpu.make_async_copy(ref, ref, sem).wait()

    def order(s):
        up = jnp.where(s < lines - 1 - line, lines - 1 - s, s - (lines - 1 - line))
        down = jnp.where(s < line, s, lines - 1 - (s - line))
        far = jnp.where(2 * line < lines, up, down)
        return jnp.where(s == lines - 1, line, far)

    relay = row_count == 4
    piece = part // 2

    def half(side):
        return pl.ds(side * piece, piece)

    def load_early(side):
        return pltpu.make_async_copy(
            early_ref.at[side], wall_ref.at[1 + side, :, half(side)], early_sem.at[side]
        )

    def rest(side):
        at = half(1 - side)
        return remote(wall_ref.at[0, :, at], wall_ref.at[1 + side, :, at], w_send.at[1 + side],
                      w_recv.at[1 + side], row_peer(row, 1 + side, row_count), col)

    def relayed(side):
        at = half(side)
        return remote(wall_ref.at[1 + side, :, at], wall_ref.at[3, :, at], w_send.at[3 + side],
                      w_recv.at[3 + side], row_peer(row, 2 - side, row_count), col)

    fetch_w = pltpu.make_async_copy(w_ref, wall_ref.at[0], w_local)
    fetch_w.start()
    if relay:
        load_early(0).start()
        load_early(1).start()

    def fetch(i):
        slot = lax.rem(i, 2)
        return pltpu.make_async_copy(
            pixels_ref.at[pl.ds(i * blocks, blocks)], pbuf_ref.at[slot], p_sem.at[slot]
        )

    def q_row(s, side):
        return 2 * order(s) + (core if side else 1 - core)

    def fetch_q(s):
        for side in range(2):
            mine = q_row(s, side)
            first = lax.rem(mine, per_line) * tile_rows
            lane = pl.multiple_of(lax.div(mine, per_line) * tile_cols, tile_cols)
            for c in range(tile_rows):
                pltpu.make_async_copy(
                    pixels_ref.at[row * col_count + first + c, pl.ds(lane, tile_cols), :],
                    qbuf_ref.at[pl.ds(side * owned + c * tile_cols, tile_cols), :],
                    q_sem,
                ).start()

    def pick(rows, index):
        at = lax.broadcasted_iota(jnp.int32, rows.shape, 0)
        return jnp.sum(jnp.where(at == index, rows, 0.0), axis=0, keepdims=True)

    def normed(x, scale_rows, gain):
        square = jnp.sum(x * x, axis=1, keepdims=True) * (1.0 / size)
        return x * (scale_rows * lax.rsqrt(square * scale_rows * scale_rows + NORM_EPS)) * gain

    fetch(0).start()
    fetch_q(0)
    fetch_w.wait()
    if relay:
        for side in range(2):
            rest(side).start()
        for side in range(2):
            load_early(side).wait()
            relayed(side).start()
    else:
        for hop in range(1, row_count):
            remote(wall_ref.at[0], wall_ref.at[hop], w_send.at[hop], w_recv.at[hop],
                   row_peer(row, hop, row_count), col).start()
    rounds = pixels_ref.shape[0] // blocks

    def keys_values(i, carry):
        fetch(i).wait()

        @pl.when(i + 1 < rounds)
        def _():
            fetch(i + 1).start()

        p = pbuf_ref[lax.rem(i, 2)].reshape(blocks * tokens, pix)
        rstd = []
        for b in range(blocks):
            lanes = rstd_ref[i * blocks + b][0:1, :]
            rstd.append(jnp.broadcast_to(lanes, (size, tokens)).T)
        for start in range(0, 2 * head_width, wide):
            at = slice(head_width + start, head_width + start + wide)
            x = jnp.dot(p, f_ref[:, at], preferred_element_type=F32)
            for b in range(blocks):
                block = i * blocks + b
                rows = pl.ds(pl.multiple_of(lax.div(block, col_count) * tile_rows, 8), tile_rows)
                cols = pl.ds(pl.multiple_of(lax.rem(block, col_count) * tile_cols, 8), tile_cols)
                u = c_ref[cols, at][None, :, :] + r_ref[rows, at][:, None, :]
                y = x[b * tokens : (b + 1) * tokens] + u.reshape(tokens, wide)
                to = pl.ds(pl.multiple_of(block * tokens, tokens), tokens)
                for g in range(2):
                    head = start // size + g
                    z = y[:, g * size : (g + 1) * size]
                    if head < heads:
                        gain = gain_ref[1:2, head * size : (head + 1) * size]
                        z = normed(z, rstd[b], gain)
                    else:
                        z = z * rstd[b]
                    kv_ref[head, to, :] = z.astype(BF16)
        return carry

    lax.fori_loop(0, rounds, keys_values, 0)

    def attend(s):
        wait(qbuf_ref, q_sem)
        own_rows = pl.ds(pl.multiple_of(row * tile_rows, 8), tile_rows)
        sides = []
        for side in range(2):
            mine = q_row(s, side)
            cols = pl.ds(pl.multiple_of(lax.rem(mine, per_line) * owned, owned), owned)
            rstd = jnp.broadcast_to(pick(rq_ref[...], mine), (size, owned)).T
            sides.append((lax.div(mine, per_line), cols, rstd))
        step_width = wide if head_width % wide == 0 else size
        for start in range(0, head_width, step_width):
            span = slice(start, start + step_width)
            x = jnp.dot(qbuf_ref[...], f_ref[:, span], preferred_element_type=F32)
            for g in range(step_width // size):
                at = slice(start + g * size, start + (g + 1) * size)
                for side, (line_row, cols, rstd) in enumerate(sides):
                    rows = slice(side * owned, (side + 1) * owned)
                    y = x[rows, g * size : (g + 1) * size]
                    y = y + (c_ref[cols, at] + pick(r_ref[own_rows, at], line_row))
                    y = normed(y, rstd, gain_ref[0:1, at] * exp_factor)
                    q_ref[start // size + g, rows, :] = y.astype(BF16)

        @pl.when(s + 1 < lines)
        def _():
            fetch_q(s + 1)

        def one_head(h, carry):
            to = pl.ds(pl.multiple_of(h * size, size), size)
            ctx_ref[s, :, to] = attention_block(
                key_block, q_ref[h], kv_ref.at[h], kv_ref.at[heads + h]
            )
            return carry

        lax.fori_loop(0, heads, one_head, 0)

    chunk = math.gcd(part, 512)

    def project_out(n, s, j):
        slot = lax.rem(n, 2)
        dest = order(s)

        @pl.when(n >= 2)
        def _():
            wait(stage_ref.at[slot], stage_send.at[slot])

        def columns(i, carry):
            at = pl.ds(pl.multiple_of(i * chunk, chunk), chunk)
            x = jnp.dot(ctx_ref[s], wall_ref[j, :, at], preferred_element_type=F32).astype(BF16)
            stage_ref[slot, :, at] = x[:owned]
            own_ref[slot, :, at] = x[owned:]
            return carry

        lax.fori_loop(0, part // chunk, columns, 0)
        remote(stage_ref.at[slot], pair_ref.at[dest, j], stage_send.at[slot],
               pair_recv.at[dest, j], row, partner).start()

    def settle(n, s, j):
        dest = order(s)
        own = own_ref[lax.rem(n, 2)].astype(F32)
        wait(pair_ref.at[dest, j], pair_recv.at[dest, j])
        pair_ref[dest, j] = (pair_ref[dest, j].astype(F32) + own).astype(BF16)

        @pl.when(jnp.logical_and(is_end, s < lines - 1))
        def _():
            pass_on(s, j)

    def pass_on(s, j):
        dest = order(s)
        up = dest > line
        to = jnp.where(up, line + 1, line - 1)
        slot = jnp.where(jnp.logical_and(dest == to, jnp.logical_not(up)), lines, dest)

        @pl.when(jnp.logical_not(is_end))
        def _():
            wait(hop_ref.at[dest, j], hop_recv.at[dest, j])
            total = pair_ref[dest, j].astype(F32) + hop_ref[dest, j].astype(F32)
            pair_ref[dest, j] = total.astype(BF16)

        remote(pair_ref.at[dest, j], hop_ref.at[slot, j], hop_send.at[dest, j],
               hop_recv.at[slot, j], row, 2 * to + core).start()

    inner = row_count - 1

    def group_start(s):
        return s * inner

    def step(s, carry):
        attend(s)

        @pl.when(s == 0)
        def _():
            if relay:
                for side in range(2):
                    rest(side).wait_recv()
            else:
                for hop in range(1, row_count - 1):
                    wait(wall_ref.at[hop], w_recv.at[hop])

        def make(t, c):
            project_out(group_start(s) + t, s, t)

            @pl.when(t > 0)
            def _():
                settle(group_start(s) + t - 1, s, t - 1)

            return c

        lax.fori_loop(0, inner, make, 0)
        settle(group_start(s) + inner - 1, s, inner - 1)

        @pl.when(jnp.logical_and(s > 0, jnp.logical_not(is_end)))
        def _():
            def late(t, c):
                pass_on(s - 1, t)
                return c

            lax.fori_loop(0, inner, late, 0)

        return carry

    lax.fori_loop(0, lines, step, 0)
    final = row_count - 1
    if relay:
        for side in range(2):
            relayed(side).wait_recv()
    else:
        wait(wall_ref.at[final], w_recv.at[final])

    def make_last(s, c):
        project_out(group_start(lines) + s, s, final)

        @pl.when(s > 0)
        def _():
            settle(group_start(lines) + s - 1, s - 1, final)

        return c

    lax.fori_loop(0, lines, make_last, 0)
    settle(group_start(lines) + lines - 1, lines - 1, final)

    def finish(j, sender):
        to = pl.ds(pl.multiple_of(sender * part, 128), part)
        side = jnp.where(line > 0, line, lines)
        wait(hop_ref.at[side, j], hop_recv.at[side, j])

        @pl.when(is_end)
        def _():
            total = pair_ref[line, j].astype(F32) + hop_ref[side, j].astype(F32)
            out_ref[:, to] = total.astype(BF16)

        @pl.when(jnp.logical_not(is_end))
        def _():
            wait(hop_ref.at[lines, j], hop_recv.at[lines, j])
            total = pair_ref[line, j].astype(F32) + hop_ref[line, j].astype(F32)
            out_ref[:, to] = (total + hop_ref[lines, j].astype(F32)).astype(BF16)

    def sender_of(hop):
        if hop == 0:
            return row
        if row_count == 4:
            return row_peer(row, hop, row_count)
        return lax.rem(row + row_count - hop, row_count)

    for j in range(row_count - 1):
        finish(j, sender_of(j))

    @pl.when(jnp.logical_not(is_end))
    def _():
        def late(s, c):
            pass_on(s, final)
            return c

        lax.fori_loop(0, lines - 1, late, 0)

    finish(final, sender_of(final))
    if relay:
        for side in range(2):
            rest(side).wait_send()
            relayed(side).wait_send()
    else:
        for hop in range(1, row_count):
            wait(wall_ref.at[0], w_send.at[hop])
    for slot in range(2):
        wait(stage_ref.at[slot], stage_send.at[slot])

    def drain(s, c):
        for j in range(row_count):
            wait(pair_ref.at[order(s), j], hop_send.at[order(s), j])
        return c

    lax.fori_loop(0, lines - 1, drain, 0)


def attend(pixels, f, r, c, gain, rstd, rq, w_out, early, sizes, heads, size):
    row_count, col_count, tile_rows, tile_cols = sizes
    devices, tokens, pix = pixels.shape
    head_width, part = w_out.shape
    lines = col_count // 2
    owned = tile_cols * tile_rows
    count = devices * tokens
    blocks = math.gcd(devices, 4)
    vmem = lambda: pl.BlockSpec(memory_space=pltpu.VMEM)
    hbm = lambda: pl.BlockSpec(memory_space=pl.ANY)
    dma = pltpu.SemaphoreType.DMA
    return pl.pallas_call(
        functools.partial(attend_kernel, sizes, heads, math.gcd(count, KEY_BLOCK)),
        in_specs=[hbm(), vmem(), vmem(), vmem(), vmem(), vmem(), vmem(), hbm(), hbm()],
        out_specs=vmem(),
        out_shape=jax.ShapeDtypeStruct((owned, part * row_count), BF16),
        scratch_shapes=[
            pltpu.VMEM((2 * heads, count, size), BF16),
            pltpu.VMEM((row_count, head_width, part), BF16),
            pltpu.VMEM((2, blocks, tokens, pix), BF16),
            pltpu.VMEM((2 * owned, pix), BF16),
            pltpu.VMEM((heads, 2 * owned, size), BF16),
            pltpu.VMEM((lines, 2 * owned, head_width), BF16),
            pltpu.VMEM((lines, row_count, owned, part), BF16),
            pltpu.VMEM((lines + 1, row_count, owned, part), BF16),
            pltpu.VMEM((2, owned, part), BF16),
            pltpu.VMEM((2, owned, part), BF16),
            dma,
            dma((2,)),
            dma((row_count + 1,)),
            dma((row_count + 1,)),
            dma((2,)),
            dma,
            dma((2,)),
            dma((lines, row_count)),
            dma((lines, row_count)),
            dma((lines + 1, row_count)),
        ],
        compiler_params=pltpu.CompilerParams(
            vmem_limit_bytes=63 * 1024 * 1024, has_side_effects=True
        ),
        cost_estimate=pl.CostEstimate(
            flops=8 * owned * lines * count * head_width,
            bytes_accessed=4 * count * head_width,
            transcendentals=heads * owned * col_count * count,
        ),
        name="attend",
    )(pixels, f, r, c, gain, rstd, rq, w_out, early)


def local(patches, w_patch, patch_bias, ln_gain, w_qkv, qk_gain, w_out):
    tile_rows, tile_cols, pix = patches.shape
    model_width = w_patch.shape[1]
    heads, size = w_qkv.shape[2], w_qkv.shape[3]
    head_width = heads * size
    col_count, row_count = lax.axis_size("col"), lax.axis_size("row")
    sizes = (row_count, col_count, tile_rows, tile_cols)
    grid_rows, grid_cols = tile_rows * row_count, tile_cols * col_count
    assert grid_cols % (tile_rows * tile_cols) == 0
    bias = patch_bias.astype(F32)[None, :]
    gain = ln_gain.astype(F32)[None, :]
    table = sincos_half(jnp.arange(max(grid_rows, grid_cols), dtype=jnp.int32), model_width)
    heads_w = w_qkv.transpose(1, 2, 0, 3).reshape(3 * heads, model_width, size)
    out_rows = w_out.reshape(head_width, -1)
    f, r, c, pixels, rstd, early = prep(
        patches.reshape(-1, pix), w_patch, gain, bias, table, heads_w, out_rows, sizes, heads,
        grid_rows, grid_cols
    )
    rq = rstd[:, 0, :].reshape(row_count, col_count, tile_rows, tile_cols)
    rq = lax.dynamic_index_in_dim(rq, lax.axis_index("row"), 0, keepdims=False)
    rq = rq.transpose(1, 0, 2).reshape(col_count, tile_rows * tile_cols)
    gains = qk_gain.reshape(2, head_width)
    return attend(
        pixels, f, r, c, gains, rstd, rq, out_rows, early, sizes, heads, size
    )


def solution(mesh):
    return jax.shard_map(
        local,
        mesh=mesh,
        in_specs=(
            P("row", "col", None),
            P(),
            P(),
            P(),
            P(None, None, "col", None),
            P(None, "col", None),
            P("col", None, "row"),
        ),
        out_specs=P(("row", "col"), None),
        check_vma=False,
    )
```
